8 devices in a mesh: dp: 1 (over z), ep: 8 (over y, x, core).
Axes of the slice: x: 2, y: 2, z: 1, core: 2. Of those that a mesh axis runs over, the one named last changes fastest.
Arguments:
- x_in: bfloat16 [512, 1536], P(('dp', 'ep'))
- expert_ids: int32 [512, 8], P(('dp', 'ep'))
- gate_val: float32 [512, 8], P(('dp', 'ep'))
- w_gate: bfloat16 [128, 1536, 512], P('ep')
- w_up: bfloat16 [128, 1536, 512], P('ep')
- w_down: bfloat16 [128, 512, 1536], P('ep')
- old_map: int32 [128], replicated
- mig_src: int32 [2], replicated
- mig_dst: int32 [2], replicated
Outputs:
- output 1: bfloat16 [512, 1536], P(('dp', 'ep'))
- output 2: bfloat16 [128, 1536, 512], P('ep')
- output 3: bfloat16 [128, 1536, 512], P('ep')
- output 4: bfloat16 [128, 512, 1536], P('ep')
All inputs are finite; a program needn't handle non-finite values.
Results may differ from the reference program's by a relative error of at most 0.001.
Values are sent between devices in bfloat16 or wider.
A program may use at most 1 GiB of HBM per device.

```python
import jax
import jax.numpy as jnp
from jax import lax

TOK_DEV = 64
TOP = 8
D = 1536
FF = 512
GROUP = 8
SLOTS = 16
MOVES = 2

EXPERTS = GROUP * SLOTS
CAP = 2 * TOK_DEV * TOP // EXPERTS
ROWS = GROUP * TOK_DEV
ROWS_CAP = GROUP * CAP


def draw_routing(key):
    num_pairs = EXPERTS // 2
    share = TOK_DEV * TOP // EXPERTS
    key_order, key_dev = jax.random.split(key)
    order = jax.random.permutation(key_order, EXPERTS)

    def one_device(dev_key, dev_index):
        key_delta, key_rows = jax.random.split(dev_key)
        delta = jax.random.randint(key_delta, (num_pairs,), 0, share)
        forced = jnp.arange(num_pairs) == dev_index % num_pairs
        delta = jnp.where(forced, share, delta)
        counts = jnp.stack([share + delta, share - delta], axis=1).reshape(EXPERTS)
        bounds = jnp.cumsum(counts)
        picks = jnp.searchsorted(bounds, jnp.arange(TOK_DEV * TOP), side='right')
        table = order[picks].reshape(TOP, TOK_DEV).T
        return table[jax.random.permutation(key_rows, TOK_DEV)]

    dev_keys = jax.random.split(key_dev, GROUP)
    expert_tab = jax.vmap(one_device)(dev_keys, jnp.arange(GROUP))
    return expert_tab.reshape(ROWS, TOP).astype(jnp.int32)


def draw_layout(key):
    key_old, key_sel = jax.random.split(key)
    old_map = jax.random.permutation(key_old, EXPERTS).astype(jnp.int32)
    chosen = jax.random.permutation(key_sel, EXPERTS)[:MOVES].astype(jnp.int32)
    return old_map, jnp.roll(chosen, -1), chosen


def setup_inputs(seed: int = 0, part: int = 0) -> dict:
    key_w = jax.random.split(jax.random.key(seed), 4)
    key_p = jax.random.split(jax.random.fold_in(jax.random.key(seed + 1), part), 3)
    x_in = jax.random.normal(key_p[0], (ROWS, D), jnp.float32).astype(jnp.bfloat16)
    expert_ids = draw_routing(key_p[1])
    gate_val = jax.random.uniform(key_p[2], (ROWS, TOP), jnp.float32, 0.5, 1.5) * TOP ** -0.5
    w_gate = (jax.random.normal(key_w[0], (EXPERTS, D, FF), jnp.float32) * D ** -0.5).astype(jnp.bfloat16)
    w_up = (jax.random.normal(key_w[1], (EXPERTS, D, FF), jnp.float32) * D ** -0.5).astype(jnp.bfloat16)
    w_down = (jax.random.normal(key_w[2], (EXPERTS, FF, D), jnp.float32) * FF ** -0.5).astype(jnp.bfloat16)
    old_map, mig_src, mig_dst = draw_layout(key_w[3])
    return {'x_in': x_in, 'expert_ids': expert_ids, 'gate_val': gate_val, 'w_gate': w_gate, 'w_up': w_up, 'w_down': w_down, 'old_map': old_map, 'mig_src': mig_src, 'mig_dst': mig_dst}


def reference(x_in, expert_ids, gate_val, w_gate, w_up, w_down, old_map, mig_src, mig_dst):
    slot_of = jnp.argsort(old_map)
    flat_ids = expert_ids.reshape(-1)
    hit_mask = (flat_ids[:, None] == jnp.arange(EXPERTS)[None, :]).astype(jnp.int32)
    rank_in = jnp.sum(jnp.cumsum(hit_mask, axis=0) * hit_mask, axis=1) - 1
    cell_pos = flat_ids * ROWS_CAP + rank_in
    tok_of = jnp.arange(ROWS * TOP) // TOP
    tok_tab = jnp.zeros((EXPERTS * ROWS_CAP,), jnp.int32).at[cell_pos].set(tok_of).reshape(EXPERTS, ROWS_CAP)
    gate_tab = jnp.zeros((EXPERTS * ROWS_CAP,), jnp.float32).at[cell_pos].set(gate_val.reshape(-1)).reshape(EXPERTS, ROWS_CAP)

    def add_expert(acc_sum, expert):
        slot = slot_of[expert]
        rows = x_in[tok_tab[expert]]
        act_g = jnp.dot(rows, w_gate[slot], preferred_element_type=jnp.float32)
        act_u = jnp.dot(rows, w_up[slot], preferred_element_type=jnp.float32)
        hidden = (jax.nn.silu(act_g) * act_u).astype(jnp.bfloat16)
        expert_out = jnp.dot(hidden, w_down[slot], preferred_element_type=jnp.float32)
        scaled = (gate_tab[expert][:, None] * expert_out).astype(jnp.bfloat16)
        return acc_sum.at[tok_tab[expert]].add(scaled.astype(jnp.float32)), expert

    acc_sum = lax.scan(add_expert, jnp.zeros((ROWS, D), jnp.float32), jnp.arange(EXPERTS))[0]
    y_out = (x_in.astype(jnp.float32) + acc_sum).astype(jnp.bfloat16)
    w_gate_new = w_gate.at[mig_dst].set(w_gate[mig_src])
    w_up_new = w_up.at[mig_dst].set(w_up[mig_src])
    w_down_new = w_down.at[mig_dst].set(w_down[mig_src])
    return (y_out, w_gate_new, w_up_new, w_down_new)
```

```python
import functools

import jax
import jax.numpy as jnp
from jax import lax
from jax.experimental import pallas as pl
from jax.experimental.pallas import tpu as pltpu
from jax.sharding import PartitionSpec as P

MESH = pl.DeviceIdType.MESH
BF16, F32 = jnp.bfloat16, jnp.float32
ANY = pl.BlockSpec(memory_space=pl.ANY)
VMEM = pl.BlockSpec(memory_space=pltpu.VMEM)
SMEM = pl.BlockSpec(memory_space=pltpu.SMEM)
LIMIT = 62 * 1024 * 1024
RING = 12
LAG = 4


def places():
    me = lax.axis_index('ep')
    core, chip = me % 2, me // 2
    x, y = chip % 2, chip // 2
    sib = chip * 2 + 1 - core
    chips = ((1 - y) * 2 + 1 - x, y * 2 + 1 - x, (1 - y) * 2 + x)
    return me, core, chip, sib, chips


def enter(partners):
    barrier = pltpu.get_barrier_semaphore()
    for dev in partners:
        pl.semaphore_signal(barrier, inc=1, device_id={'ep': dev}, device_id_type=MESH)
    pl.semaphore_wait(barrier, len(partners))


def remote(src, dst, send, recv, dev):
    return pltpu.make_async_remote_copy(src, dst, send, recv, device_id={'ep': dev}, device_id_type=MESH)


def dispatch_kernel(x_ref, meta_ref, xall, mall, send, recv):
    me, core, chip, sib, chips = places()
    peers = [c * 2 + core for c in chips]
    enter(peers + [sib])

    def pair(k, src_x, src_m, block, dev):
        return (remote(src_x, xall.at[block], send.at[2 * k], recv.at[2 * k], dev),
                remote(src_m, mall.at[block], send.at[2 * k + 1], recv.at[2 * k + 1], dev))

    first = [pair(k, x_ref, meta_ref, me, peers[k]) for k in range(3)]
    first.append(pair(3, x_ref, meta_ref, me, sib))
    for group in first:
        for copy in group:
            copy.start()
    xall[pl.ds(me, 1)] = x_ref[...][None]
    mall[pl.ds(me, 1)] = meta_ref[...][None]
    second = []
    for k in (1, 2, 0):
        for copy in first[k]:
            copy.wait_recv()
        fwd = pair(4 + k, xall.at[peers[k]], mall.at[peers[k]], peers[k], sib)
        for copy in fwd:
            copy.start()
        second.append(fwd)
    for copy in first[3]:
        copy.wait_recv()
    for group in first:
        for copy in group:
            copy.wait_send()
    for group in second:
        for copy in group:
            copy.wait()


def gate_up_kernel(old_map, x_ref, mall, wg, wu, wg_new, wu_new, z_ref, at_ref, gr_ref,
                   bg, bu, xg, a_ref, pos, gsc, meta, sem_in, sem_out):
    me = lax.axis_index('ep')
    slots = wg.shape[0]
    devs, tok = x_ref.shape[0] // 64, 64
    total = devs * tok
    cap = 8
    rows = devs * cap

    def load(s):
        b = lax.rem(s, RING)
        return (pltpu.make_async_copy(wg.at[s], bg.at[b], sem_in.at[0, b]),
                pltpu.make_async_copy(wu.at[s], bu.at[b], sem_in.at[1, b]))

    def drain(s):
        b = lax.rem(s, RING)
        return (pltpu.make_async_copy(bg.at[b], wg_new.at[s], sem_out.at[0, b]),
                pltpu.make_async_copy(bu.at[b], wu_new.at[s], sem_out.at[1, b]))

    for s in range(RING):
        for copy in load(s):
            copy.start()

    lane = lax.broadcasted_iota(jnp.int32, (16, 128), 1)
    for p in range(devs // 2):
        other = pltpu.roll(mall[2 * p + 1], 64, axis=1)
        meta[:, pl.ds(128 * p, 128)] = jnp.where(lane < 64, mall[2 * p], other)
    ids = meta[0:8, :]
    gates = meta[8:16, :]
    hits, gs = [], []
    for j in range(slots):
        same = ids == old_map[me * slots + j].astype(F32)
        hits.append(jnp.sum(jnp.where(same, 1.0, 0.0), axis=0, keepdims=True))
        gs.append(jnp.sum(jnp.where(same, gates, 0.0), axis=0, keepdims=True))
    hit = jnp.concatenate(hits, axis=0)
    gsc[...] = jnp.concatenate(gs, axis=0)
    t_row = lax.broadcasted_iota(jnp.int32, (total, total), 0)
    t_col = lax.broadcasted_iota(jnp.int32, (total, total), 1)
    before = jnp.where((t_row < t_col) & (t_row // tok == t_col // tok), 1.0, 0.0).astype(BF16)
    rank = jnp.dot(hit.astype(BF16), before, preferred_element_type=F32)
    owner = (lax.broadcasted_iota(jnp.int32, (slots, total), 1) // tok * cap).astype(F32)
    pos[...] = jnp.where(hit > 0.5, rank + owner, -1.0)
    post = jnp.transpose(jnp.concatenate([pos[...], jnp.full((128 - slots, total), -1.0, F32)], axis=0))
    wide = lax.broadcasted_iota(jnp.int32, (total, 128), 1)
    for p in range(slots // 2):
        want = jnp.where(wide < rows, post[:, 2 * p:2 * p + 1], post[:, 2 * p + 1:2 * p + 2])
        at_ref[:, pl.ds(128 * p, 128)] = jnp.where(want == (wide % rows).astype(F32), 1.0, 0.0).astype(BF16)

    row_id = lax.broadcasted_iota(jnp.int32, (rows, total), 0).astype(F32)

    @pl.loop(0, slots)
    def _(j):
        r0 = pl.multiple_of(j * rows, rows)
        chosen = row_id == pos[pl.ds(j, 1), :]
        a_ref[pl.ds(r0, rows), :] = jnp.where(chosen, 1.0, 0.0).astype(BF16)
        g = jnp.sum(jnp.where(chosen, gsc[pl.ds(j, 1), :], 0.0), axis=1, keepdims=True)
        gr_ref[pl.ds(r0, rows), :] = jnp.broadcast_to(g, (rows, 128))

    @pl.loop(0, slots // 4)
    def _(q):
        r0 = pl.multiple_of(q * 4 * rows, 4 * rows)
        picked = jnp.dot(a_ref[pl.ds(r0, 4 * rows), :], x_ref[...], preferred_element_type=F32)
        xg[pl.ds(r0, 4 * rows), :] = picked.astype(BF16)

    @pl.loop(0, slots)
    def _(s):
        b = lax.rem(s, RING)
        for copy in load(s):
            copy.wait()
        for copy in drain(s):
            copy.start()
        r0 = pl.multiple_of(s * rows, rows)
        xs = xg[pl.ds(r0, rows), :]
        act_g = jnp.dot(xs, bg[b], preferred_element_type=F32)
        act_u = jnp.dot(xs, bu[b], preferred_element_type=F32)
        z_ref[pl.ds(r0, rows), :] = (jax.nn.silu(act_g) * act_u).astype(BF16)

        @pl.when((s >= LAG) & (s - LAG + RING < slots))
        def _():
            for copy in drain(s - LAG):
                copy.wait()
            for copy in load(s - LAG + RING):
                copy.start()

    for s in range(max(slots - RING, 0), slots):
        for copy in drain(s):
            copy.wait()


def down_kernel(z_ref, at_ref, gr_ref, wd, wd_new, out_ref, bd, c_ref, sem_in, sem_out):
    slots = wd.shape[0]
    rows = z_ref.shape[0] // slots

    def load(s):
        return pltpu.make_async_copy(wd.at[s], bd.at[s], sem_in.at[s])

    def drain(s):
        return pltpu.make_async_copy(bd.at[s], wd_new.at[s], sem_out.at[s])

    for s in range(slots):
        load(s).start()

    @pl.loop(0, slots)
    def _(s):
        load(s).wait()
        drain(s).start()
        r0 = pl.multiple_of(s * rows, rows)
        o = jnp.dot(z_ref[pl.ds(r0, rows), :], bd[s], preferred_element_type=F32)
        c_ref[pl.ds(r0, rows), :] = (o * gr_ref[pl.ds(r0, rows), 0:1]).astype(BF16)

    cols = 256

    @pl.loop(0, out_ref.shape[1] // cols)
    def _(n):
        c0 = pl.multiple_of(n * cols, cols)
        out_ref[:, pl.ds(c0, cols)] = jnp.dot(at_ref[...], c_ref[:, pl.ds(c0, cols)], preferred_element_type=F32)

    @pl.loop(0, slots)
    def _(s):
        drain(s).wait()


def combine_kernel(part, x_ref, y_ref, near, summed, far, send, recv):
    me, core, chip, sib, chips = places()
    peers = [c * 2 + core for c in chips]
    order = list(chips) + [chip]
    enter(peers + [sib])
    across = [remote(part.at[c * 2 + 1 - core], near.at[k], send.at[k], recv.at[k], sib) for k, c in enumerate(order)]
    for copy in across:
        copy.start()
    out = [remote(summed.at[k], far.at[k], send.at[4 + k], recv.at[4 + k], peers[k]) for k in range(3)]
    for k in range(4):
        across[k].wait_recv()
        summed[k] = part[order[k] * 2 + core] + near[k]
        if k >= 1:
            out[k - 1].start()
    acc = x_ref[...].astype(F32) + summed[3]
    for k in (1, 2, 0):
        out[k].wait_recv()
        acc = acc + far[k]
    y_ref[...] = acc.astype(BF16)
    for copy in across + out:
        copy.wait_send()


def patch_kernel(src, dst, half, other, wg, wu, wd, wg_old, wu_old, wd_old, wg_new, wu_new, wd_new, buf, sem):
    me = lax.axis_index('ep')
    core = me % 2
    slots = wg.shape[0]
    depth, width = wg.shape[1:]
    part = half.shape[0] * half.shape[1]
    here = [dst[i] // slots == me for i in range(2)]
    local = here[0] & here[1]

    def run(copies):
        for copy in copies:
            copy.start()
        for copy in copies:
            copy.wait()

    def put(slot):
        copies = [pltpu.make_async_copy(buf.at[pl.ds(0, depth)], wg_new.at[slot], sem.at[0]),
                  pltpu.make_async_copy(buf.at[pl.ds(depth, depth)], wu_new.at[slot], sem.at[1])]
        for b in range(depth // width):
            copies.append(pltpu.make_async_copy(buf.at[pl.ds(2 * depth + width * b, width)],
                                                wd_new.at[slot, :, pl.ds(width * b, width)], sem.at[2 + b]))
        run(copies)

    @pl.when((here[0] | here[1]) & jnp.logical_not(local))
    def _():
        slot = jnp.where(here[0], dst[0], dst[1]) % slots
        size = half.shape[1]
        copies = []
        for p in range(2):
            copies.append(pltpu.make_async_copy(
                half.at[p], buf.at[pl.ds(pl.multiple_of(core * part + p * size, 128), size)], sem.at[p]))
            copies.append(pltpu.make_async_copy(
                other.at[p], buf.at[pl.ds(pl.multiple_of((1 - core) * part + p * size, 128), size)], sem.at[2 + p]))
        run(copies)
        put(slot)

    @pl.when(local)
    def _():
        for i in range(2):
            s = src[i] % slots
            copies = [pltpu.make_async_copy(wg.at[s], buf.at[pl.ds(0, depth)], sem.at[0]),
                      pltpu.make_async_copy(wu.at[s], buf.at[pl.ds(depth, depth)], sem.at[1])]
            for b in range(depth // width):
                copies.append(pltpu.make_async_copy(wd.at[s, :, pl.ds(width * b, width)],
                                                    buf.at[pl.ds(2 * depth + width * b, width)], sem.at[2 + b]))
            run(copies)
            put(dst[i] % slots)


def solution(mesh):
    groups = mesh.shape['ep']
    chips = groups // 2
    to_sib = [(d, d + 1 - 2 * (d % 2)) for d in range(groups)]

    def flip(bit):
        return [(d, d + bit - 2 * bit * ((d // bit) % 2)) for d in range(groups)]

    to_x, to_y = flip(2), flip(4)

    def migrate(w_gate, w_up, w_down, mig_src, mig_dst):
        slots, depth, width = w_gate.shape
        me = lax.axis_index('ep')
        core, chip = me % 2, me // 2
        owner = mig_src // slots
        oc = owner // 2
        i_own = (owner[0] == me) | (owner[1] == me)
        chip_own = (oc[0] == chip) | (oc[1] == chip)
        loc = jnp.where(owner[0] == me, mig_src[0], mig_src[1]) % slots
        same_chip = oc[0] == oc[1]
        same_x, same_y = oc[0] % 2 == oc[1] % 2, oc[0] // 2 == oc[1] // 2
        down = lax.dynamic_index_in_dim(w_down, loc, 0, keepdims=False)
        mine = jnp.concatenate(
            [lax.dynamic_index_in_dim(w_gate, loc, 0, keepdims=False),
             lax.dynamic_index_in_dim(w_up, loc, 0, keepdims=False)]
            + [down[:, width * b:width * (b + 1)] for b in range(depth // width)], axis=0)
        mine = mine.reshape(4, 3 * depth // 4, width)
        near = lax.ppermute(lax.dynamic_slice_in_dim(mine, 2 - 2 * core, 2, 0), 'ep', to_sib)
        own = lax.dynamic_slice_in_dim(mine, 2 * core, 2, 0)
        held = jnp.where(i_own, own, near)
        rx1 = lax.ppermute(held[0], 'ep', to_x)
        ry1 = lax.ppermute(jnp.where(same_x, held[0], held[1]), 'ep', to_y)

        def second():
            rx2 = lax.ppermute(jnp.where(chip_own, held[1], ry1), 'ep', to_x)
            ry2 = lax.ppermute(jnp.where(chip_own, held[1], rx1), 'ep', to_y)
            along = jnp.where(same_y, jnp.stack([rx1, rx2]), jnp.where(same_x, jnp.stack([ry1, ry2]), jnp.stack([ry2, rx2])))
            other = lax.ppermute(jnp.where(same_chip, own, along), 'ep', to_sib)
            return jnp.where(same_chip, near, along), other

        return second()

    def local_step(x_loc, expert_ids, gate_val, w_gate, w_up, w_down, old_map, mig_src, mig_dst):
        tok, model = x_loc.shape
        slots, depth, width = w_gate.shape
        total = groups * tok
        rows = slots * groups * 8
        half, other = migrate(w_gate, w_up, w_down, mig_src, mig_dst)

        meta = jnp.concatenate([expert_ids.astype(F32).T, gate_val.T], axis=0)
        meta = jnp.pad(meta, ((0, 0), (0, 128 - tok)))
        xall, mall = pl.pallas_call(
            dispatch_kernel,
            out_shape=(jax.ShapeDtypeStruct((groups, tok, model), BF16), jax.ShapeDtypeStruct((groups, 16, 128), F32)),
            in_specs=[VMEM, VMEM], out_specs=(VMEM, VMEM),
            scratch_shapes=[pltpu.SemaphoreType.DMA((14,)), pltpu.SemaphoreType.DMA((14,))],
            compiler_params=pltpu.CompilerParams(collective_id=0, has_side_effects=True),
            cost_estimate=pl.CostEstimate(flops=8_000_000_000, bytes_accessed=2_000_000, transcendentals=0),
            name='dispatch',
        )(x_loc, meta)

        bytes_gu = 4 * 2 * slots * depth * width
        wg_new, wu_new, z, at, gr = pl.pallas_call(
            gate_up_kernel,
            out_shape=(jax.ShapeDtypeStruct(w_gate.shape, BF16), jax.ShapeDtypeStruct(w_up.shape, BF16),
                       jax.ShapeDtypeStruct((rows, width), BF16), jax.ShapeDtypeStruct((total, rows), BF16),
                       jax.ShapeDtypeStruct((rows, 128), F32)),
            in_specs=[SMEM, VMEM, VMEM, ANY, ANY], out_specs=(ANY, ANY, VMEM, VMEM, VMEM),
            scratch_shapes=[pltpu.VMEM((RING, depth, width), BF16), pltpu.VMEM((RING, depth, width), BF16),
                            pltpu.VMEM((rows, model), BF16), pltpu.VMEM((rows, total), BF16),
                            pltpu.VMEM((slots, total), F32), pltpu.VMEM((slots, total), F32),
                            pltpu.VMEM((16, total), F32),
                            pltpu.SemaphoreType.DMA((2, RING)), pltpu.SemaphoreType.DMA((2, RING))],
            compiler_params=pltpu.CompilerParams(vmem_limit_bytes=LIMIT),
            cost_estimate=pl.CostEstimate(flops=30_000_000_000, bytes_accessed=bytes_gu, transcendentals=0),
            name='gate_up',
        )(old_map, xall.reshape(total, model), mall, w_gate, w_up)

        wd_new, part = pl.pallas_call(
            down_kernel,
            out_shape=(jax.ShapeDtypeStruct(w_down.shape, BF16), jax.ShapeDtypeStruct((total, model), F32)),
            in_specs=[VMEM, VMEM, VMEM, ANY], out_specs=(ANY, VMEM),
            scratch_shapes=[pltpu.VMEM((slots, width, depth), BF16), pltpu.VMEM((rows, model), BF16),
                            pltpu.SemaphoreType.DMA((slots,)), pltpu.SemaphoreType.DMA((slots,))],
            compiler_params=pltpu.CompilerParams(vmem_limit_bytes=LIMIT),
            cost_estimate=pl.CostEstimate(flops=15_000_000_000, bytes_accessed=bytes_gu // 2, transcendentals=0),
            name='down',
        )(z, at, gr, w_down)

        y_out = pl.pallas_call(
            combine_kernel,
            out_shape=jax.ShapeDtypeStruct((tok, model), BF16),
            in_specs=[VMEM, VMEM], out_specs=VMEM,
            scratch_shapes=[pltpu.VMEM((4, tok, model), F32), pltpu.VMEM((4, tok, model), F32),
                            pltpu.VMEM((3, tok, model), F32),
                            pltpu.SemaphoreType.DMA((7,)), pltpu.SemaphoreType.DMA((7,))],
            compiler_params=pltpu.CompilerParams(collective_id=1, has_side_effects=True, vmem_limit_bytes=40 * 1024 * 1024),
            cost_estimate=pl.CostEstimate(flops=16_000_000_000, bytes_accessed=4_000_000, transcendentals=0),
            name='combine',
        )(part.reshape(groups, tok, model), x_loc)

        wg_new, wu_new, wd_new = pl.pallas_call(
            patch_kernel,
            out_shape=tuple(jax.ShapeDtypeStruct(w.shape, BF16) for w in (w_gate, w_up, w_down)),
            in_specs=[SMEM, SMEM] + [ANY] * 8, out_specs=(ANY, ANY, ANY),
            input_output_aliases={7: 0, 8: 1, 9: 2},
            scratch_shapes=[pltpu.VMEM((3 * depth, width), BF16), pltpu.SemaphoreType.DMA((5,))],
            cost_estimate=pl.CostEstimate(flops=3_000_000_000, bytes_accessed=9_000_000, transcendentals=0),
            name='patch',
        )(mig_src, mig_dst, half, other, w_gate, w_up, w_down, wg_new, wu_new, wd_new)
        return y_out, wg_new, wu_new, wd_new

    row_spec = P(('dp', 'ep'), None)
    slot_spec = P('ep', None, None)
    return jax.shard_map(local_step, mesh=mesh, in_specs=(row_spec, row_spec, row_spec, slot_spec, slot_spec, slot_spec, P(), P(), P()), out_specs=(row_spec, slot_spec, slot_spec, slot_spec), check_vma=False)
```

```python
import functools

import jax
import jax.numpy as jnp
from jax import lax
from jax.experimental import pallas as pl
from jax.experimental.pallas import tpu as pltpu
from jax.sharding import PartitionSpec as P

MESH = pl.DeviceIdType.MESH
BF16, F32 = jnp.bfloat16, jnp.float32
ANY = pl.BlockSpec(memory_space=pl.ANY)
VMEM = pl.BlockSpec(memory_space=pltpu.VMEM)
SMEM = pl.BlockSpec(memory_space=pltpu.SMEM)
LIMIT = 62 * 1024 * 1024
HALF = 8


def places():
    me = lax.axis_index('ep')
    core, chip = me % 2, me // 2
    x, y = chip % 2, chip // 2
    sib = chip * 2 + 1 - core
    chips = ((1 - y) * 2 + 1 - x, y * 2 + 1 - x, (1 - y) * 2 + x)
    return me, core, chip, sib, chips


def enter(partners):
    barrier = pltpu.get_barrier_semaphore()
    for dev in partners:
        pl.semaphore_signal(barrier, inc=1, device_id={'ep': dev}, device_id_type=MESH)
    pl.semaphore_wait(barrier, len(partners))


def remote(src, dst, send, recv, dev):
    return pltpu.make_async_remote_copy(src, dst, send, recv, device_id={'ep': dev}, device_id_type=MESH)


def pack_kernel(src, wg, wu, wd, send_ref, own_ref, sem):
    me = lax.axis_index('ep')
    slots, depth, width = wg.shape
    half = 3 * depth // 2
    slot = jnp.where(src[0] // slots == me, src[0], src[1]) % slots

    def first(ref, k):
        return [pltpu.make_async_copy(wg.at[slot], ref.at[pl.ds(0, depth)], sem.at[k]),
                pltpu.make_async_copy(wu.at[slot, pl.ds(0, half - depth)], ref.at[pl.ds(depth, half - depth)], sem.at[k + 1])]

    def second(ref, k):
        rest = 2 * depth - half
        copies = [pltpu.make_async_copy(wu.at[slot, pl.ds(half - depth, rest)], ref.at[pl.ds(0, rest)], sem.at[k])]
        for b in range(depth // width):
            copies.append(pltpu.make_async_copy(wd.at[slot, :, pl.ds(width * b, width)],
                                                ref.at[pl.ds(rest + width * b, width)], sem.at[k + 1 + b]))
        return copies

    def run(copies):
        for copy in copies:
            copy.start()
        for copy in copies:
            copy.wait()

    @pl.when(me % 2 == 0)
    def _():
        run(second(send_ref, 2) + first(own_ref, 0))

    @pl.when(me % 2 == 1)
    def _():
        run(first(send_ref, 0) + second(own_ref, 2))


def dispatch_kernel(x_ref, meta_ref, slot_ref, xall, mall, near, send, recv):
    me, core, chip, sib, chips = places()
    peers = [c * 2 + core for c in chips]
    enter(peers + [sib])

    def pair(k, src_x, src_m, block, dev):
        return (remote(src_x, xall.at[block], send.at[2 * k], recv.at[2 * k], dev),
                remote(src_m, mall.at[block], send.at[2 * k + 1], recv.at[2 * k + 1], dev))

    first = [pair(k, x_ref, meta_ref, me, peers[k]) for k in range(3)]
    first.append(pair(3, x_ref, meta_ref, me, sib))
    for group in first:
        for copy in group:
            copy.start()
    slot = remote(slot_ref, near, send.at[14], recv.at[14], sib)
    slot.start()
    xall[pl.ds(me, 1)] = x_ref[...][None]
    mall[pl.ds(me, 1)] = meta_ref[...][None]
    second = []
    for k in (1, 2, 0):
        for copy in first[k]:
            copy.wait_recv()
        fwd = pair(4 + k, xall.at[peers[k]], mall.at[peers[k]], peers[k], sib)
        for copy in fwd:
            copy.start()
        second.append(fwd)
    for copy in first[3]:
        copy.wait_recv()
    for group in first:
        for copy in group:
            copy.wait_send()
    for group in second:
        for copy in group:
            copy.wait()
    slot.wait()


def stream(slots0, count, w, w_new, bufs, sem_in, sem_out):
    def load(i):
        return [pltpu.make_async_copy(w[k].at[slots0 + i], bufs[k].at[i], sem_in.at[k, i]) for k in range(3)]

    def drain(i):
        return [pltpu.make_async_copy(bufs[k].at[i], w_new[k].at[slots0 + i], sem_out.at[k, i]) for k in range(3)]

    return load, drain


def experts(i, xs, gate, bufs):
    act_g = jnp.dot(xs, bufs[0][i], preferred_element_type=F32)
    act_u = jnp.dot(xs, bufs[1][i], preferred_element_type=F32)
    z = (jax.nn.silu(act_g) * act_u).astype(BF16)
    o = jnp.dot(z, bufs[2][i], preferred_element_type=F32)
    return (o * gate).astype(BF16)


def first_kernel(old_map, x_hbm, m_hbm, wg, wu, wd, wg_new, wu_new, wd_new, xg_out, at_out, gr_out, c_out,
                 bg, bu, bd, x_ref, mall, xg, a_ref, at_ref, gr_ref, c_ref, pos, gsc, meta, sem_in, sem_out, sem):
    me = lax.axis_index('ep')
    slots, tok, cap = wg.shape[0], 64, 8
    total = x_ref.shape[0]
    devs = total // tok
    rows = devs * cap
    bufs = (bg, bu, bd)
    load, drain = stream(0, HALF, (wg, wu, wd), (wg_new, wu_new, wd_new), bufs, sem_in, sem_out)
    get_m = pltpu.make_async_copy(m_hbm, mall, sem.at[0])
    get_x = pltpu.make_async_copy(x_hbm, x_ref, sem.at[1])
    get_m.start()
    get_x.start()
    for i in range(HALF):
        for copy in load(i):
            copy.start()
    get_m.wait()

    lane = lax.broadcasted_iota(jnp.int32, (16, 128), 1)
    for p in range(devs // 2):
        other = pltpu.roll(mall[2 * p + 1], 64, axis=1)
        meta[:, pl.ds(128 * p, 128)] = jnp.where(lane < 64, mall[2 * p], other)
    ids = meta[0:8, :]
    gates = meta[8:16, :]
    hits, gs = [], []
    for j in range(slots):
        same = ids == old_map[me * slots + j].astype(F32)
        hits.append(jnp.sum(jnp.where(same, 1.0, 0.0), axis=0, keepdims=True))
        gs.append(jnp.sum(jnp.where(same, gates, 0.0), axis=0, keepdims=True))
    hit = jnp.concatenate(hits, axis=0)
    gsc[...] = jnp.concatenate(gs, axis=0)
    t_row = lax.broadcasted_iota(jnp.int32, (total, total), 0)
    t_col = lax.broadcasted_iota(jnp.int32, (total, total), 1)
    before = jnp.where((t_row < t_col) & (t_row // tok == t_col // tok), 1.0, 0.0).astype(BF16)
    rank = jnp.dot(hit.astype(BF16), before, preferred_element_type=F32)
    owner = (lax.broadcasted_iota(jnp.int32, (slots, total), 1) // tok * cap).astype(F32)
    pos[...] = jnp.where(hit > 0.5, rank + owner, -1.0)
    post = jnp.transpose(jnp.concatenate([pos[...], jnp.full((128 - slots, total), -1.0, F32)], axis=0))
    wide = lax.broadcasted_iota(jnp.int32, (total, 128), 1)
    for p in range(slots // 2):
        want = jnp.where(wide < rows, post[:, 2 * p:2 * p + 1], post[:, 2 * p + 1:2 * p + 2])
        at_ref[:, pl.ds(128 * p, 128)] = jnp.where(want == (wide % rows).astype(F32), 1.0, 0.0).astype(BF16)

    row_id = lax.broadcasted_iota(jnp.int32, (rows, total), 0).astype(F32)

    @pl.loop(0, slots)
    def _(j):
        r0 = pl.multiple_of(j * rows, rows)
        chosen = row_id == pos[pl.ds(j, 1), :]
        a_ref[pl.ds(r0, rows), :] = jnp.where(chosen, 1.0, 0.0).astype(BF16)
        g = jnp.sum(jnp.where(chosen, gsc[pl.ds(j, 1), :], 0.0), axis=1, keepdims=True)
        gr_ref[pl.ds(r0, rows), :] = jnp.broadcast_to(g, (rows, 128))

    get_x.wait()

    @pl.loop(0, slots // 4)
    def _(q):
        r0 = pl.multiple_of(q * 4 * rows, 4 * rows)
        picked = jnp.dot(a_ref[pl.ds(r0, 4 * rows), :], x_ref[...], preferred_element_type=F32)
        xg[pl.ds(r0, 4 * rows), :] = picked.astype(BF16)

    @pl.loop(0, HALF)
    def _(i):
        for copy in load(i):
            copy.wait()
        for copy in drain(i):
            copy.start()
        r0 = pl.multiple_of(i * rows, rows)
        c_ref[pl.ds(r0, rows), :] = experts(i, xg[pl.ds(r0, rows), :], gr_ref[pl.ds(r0, rows), 0:1], bufs)

    done = HALF * rows
    puts = [pltpu.make_async_copy(xg.at[pl.ds(done, slots * rows - done)], xg_out, sem.at[0]),
            pltpu.make_async_copy(at_ref, at_out, sem.at[1]),
            pltpu.make_async_copy(gr_ref.at[pl.ds(done, slots * rows - done)], gr_out, sem.at[2]),
            pltpu.make_async_copy(c_ref, c_out, sem.at[3])]
    for copy in puts:
        copy.start()
    for i in range(HALF):
        for copy in drain(i):
            copy.wait()
    for copy in puts:
        copy.wait()


def second_kernel(xg_hbm, at_hbm, gr_hbm, c_hbm, wg, wu, wd, wg_old, wu_old, wd_old, wg_new, wu_new, wd_new, out_hbm,
                  bg, bu, bd, xg, at_ref, gr_ref, c_ref, out_ref, sem_in, sem_out, sem):
    slots = wg.shape[0]
    count = slots - HALF
    rows = xg.shape[0] // count
    bufs = (bg, bu, bd)
    load, drain = stream(HALF, count, (wg, wu, wd), (wg_new, wu_new, wd_new), bufs, sem_in, sem_out)
    done = HALF * rows
    gets = [pltpu.make_async_copy(xg_hbm, xg, sem.at[0]), pltpu.make_async_copy(gr_hbm, gr_ref, sem.at[1]),
            pltpu.make_async_copy(c_hbm, c_ref.at[pl.ds(0, done)], sem.at[2]), pltpu.make_async_copy(at_hbm, at_ref, sem.at[3])]
    for copy in gets[:2]:
        copy.start()
    for i in range(count):
        for copy in load(i):
            copy.start()
    for copy in gets[2:]:
        copy.start()
    for copy in gets[:2]:
        copy.wait()

    @pl.loop(0, count)
    def _(i):
        for copy in load(i):
            copy.wait()
        for copy in drain(i):
            copy.start()
        r0 = pl.multiple_of(i * rows, rows)
        c = experts(i, xg[pl.ds(r0, rows), :], gr_ref[pl.ds(r0, rows), 0:1], bufs)
        c_ref[pl.ds(pl.multiple_of(done + i * rows, rows), rows), :] = c

    for copy in gets[2:]:
        copy.wait()
    cols = 256

    @pl.loop(0, out_ref.shape[1] // cols)
    def _(n):
        c0 = pl.multiple_of(n * cols, cols)
        out_ref[:, pl.ds(c0, cols)] = jnp.dot(at_ref[...], c_ref[:, pl.ds(c0, cols)], preferred_element_type=F32)

    put = pltpu.make_async_copy(out_ref, out_hbm, sem.at[0])
    put.start()
    for i in range(count):
        for copy in drain(i):
            copy.wait()
    put.wait()


def combine_kernel(part, x_ref, rx1, ry1, rx2, ry2, own, y_ref, got, gown, here, near, summed, far, sem, send, recv):
    me, core, chip, sib, chips = places()
    peers = [c * 2 + core for c in chips]
    order = list(chips) + [chip]
    mine = [pltpu.make_async_copy(part.at[c * 2 + core], here.at[k], sem.at[k]) for k, c in enumerate(order)]
    for copy in mine:
        copy.start()
    enter(peers + [sib])
    across = [remote(part.at[c * 2 + 1 - core], near.at[k], send.at[k], recv.at[k], sib) for k, c in enumerate(order)]
    for copy in across:
        copy.start()
    out = [remote(summed.at[k], far.at[k], send.at[4 + k], recv.at[4 + k], peers[k]) for k in range(3)]
    moved = [remote(r, got.at[k], send.at[7 + k], recv.at[7 + k], sib) for k, r in enumerate((rx1, ry1, rx2, ry2))]
    moved.append(remote(own, gown, send.at[11], recv.at[11], sib))
    for copy in moved:
        copy.start()
    for k in range(4):
        mine[k].wait()
        across[k].wait_recv()
        summed[k] = here[k] + near[k]
        if k >= 1:
            out[k - 1].start()
    acc = x_ref[...].astype(F32) + summed[3]
    for k in (1, 2, 0):
        out[k].wait_recv()
        acc = acc + far[k]
    y_ref[...] = acc.astype(BF16)
    for copy in moved:
        copy.wait_recv()
    for copy in across + out + moved:
        copy.wait_send()


def patch_kernel(src, dst, rx1, ry1, rx2, ry2, got, near, gown, wg, wu, wd, wg_old, wu_old, wd_old,
                 wg_new, wu_new, wd_new, buf, sem):
    me = lax.axis_index('ep')
    core = me % 2
    slots, depth, width = wg.shape
    part = rx1.shape[0]
    owner = [dst[i] // slots for i in range(2)]
    here = [owner[i] == me for i in range(2)]
    chip = [owner[i] // 2 for i in range(2)]
    local = here[0] & here[1]
    comes = (here[0] | here[1]) & jnp.logical_not(local)
    same_x, same_y = chip[0] % 2 == chip[1] % 2, chip[0] // 2 == chip[1] // 2

    def run(copies):
        for copy in copies:
            copy.start()
        for copy in copies:
            copy.wait()

    def put(slot):
        copies = [pltpu.make_async_copy(buf.at[pl.ds(0, depth)], wg_new.at[slot], sem.at[0]),
                  pltpu.make_async_copy(buf.at[pl.ds(depth, depth)], wu_new.at[slot], sem.at[1])]
        for b in range(depth // width):
            copies.append(pltpu.make_async_copy(buf.at[pl.ds(2 * depth + width * b, width)],
                                                wd_new.at[slot, :, pl.ds(width * b, width)], sem.at[2 + b]))
        run(copies)

    def receive(case, a0, a1, b0, b1):
        @pl.when(comes & case)
        def _():
            copies = []
            for p, (a, b) in enumerate(((a0, b0), (a1, b1))):
                at = pl.multiple_of(core * 2 * part + p * part, 128)
                copies.append(pltpu.make_async_copy(a, buf.at[pl.ds(at, part)], sem.at[p]))
                at = pl.multiple_of((1 - core) * 2 * part + p * part, 128)
                copies.append(pltpu.make_async_copy(b, buf.at[pl.ds(at, part)], sem.at[2 + p]))
            run(copies)

    other = jnp.logical_not
    rows = pl.ds(0, part), pl.ds(part, part)
    receive(same_y & same_x, near.at[rows[0]], near.at[rows[1]], gown.at[rows[0]], gown.at[rows[1]])
    receive(same_y & other(same_x), rx1, rx2, got.at[0], got.at[2])
    receive(same_x & other(same_y), ry2, ry1, got.at[3], got.at[1])
    receive(other(same_x) & other(same_y), ry2, rx2, got.at[3], got.at[2])

    @pl.when(comes)
    def _():
        put(jnp.where(here[0], dst[0], dst[1]) % slots)

    @pl.when(local)
    def _():
        for i in range(2):
            s = src[i] % slots
            copies = [pltpu.make_async_copy(wg.at[s], buf.at[pl.ds(0, depth)], sem.at[0]),
                      pltpu.make_async_copy(wu.at[s], buf.at[pl.ds(depth, depth)], sem.at[1])]
            for b in range(depth // width):
                copies.append(pltpu.make_async_copy(wd.at[s, :, pl.ds(width * b, width)],
                                                    buf.at[pl.ds(2 * depth + width * b, width)], sem.at[2 + b]))
            run(copies)
            put(dst[i] % slots)


def cost(flops, moved):
    return pl.CostEstimate(flops=flops, bytes_accessed=moved, transcendentals=0)


def solution(mesh):
    groups = mesh.shape['ep']

    def flip(bit):
        return [(d, d + bit - 2 * bit * ((d // bit) % 2)) for d in range(groups)]

    to_x, to_y = flip(2), flip(4)

    def local_step(x_loc, expert_ids, gate_val, w_gate, w_up, w_down, old_map, mig_src, mig_dst):
        tok, model = x_loc.shape
        slots, depth, width = w_gate.shape
        total = groups * tok
        per = groups * 8
        rows = slots * per
        later = (slots - HALF) * per
        half = 3 * depth // 2
        weights = (w_gate, w_up, w_down)
        shapes = tuple(jax.ShapeDtypeStruct(w.shape, BF16) for w in weights)
        dma = pltpu.SemaphoreType.DMA
        slot_bytes = 6 * depth * width

        send, own = pl.pallas_call(
            pack_kernel,
            out_shape=(jax.ShapeDtypeStruct((half, width), BF16),) * 2,
            in_specs=[SMEM, ANY, ANY, ANY], out_specs=(VMEM, VMEM),
            scratch_shapes=[dma((6,))],
            cost_estimate=cost(2_000_000_000, 2 * slot_bytes), name='pack',
        )(mig_src, *weights)

        meta = jnp.concatenate([expert_ids.astype(F32).T, gate_val.T], axis=0)
        meta = jnp.pad(meta, ((0, 0), (0, 128 - tok)))
        xall, mall, near = pl.pallas_call(
            dispatch_kernel,
            out_shape=(jax.ShapeDtypeStruct((groups, tok, model), BF16), jax.ShapeDtypeStruct((groups, 16, 128), F32),
                       jax.ShapeDtypeStruct((half, width), BF16)),
            in_specs=[VMEM, VMEM, ANY], out_specs=(VMEM, VMEM, ANY),
            scratch_shapes=[dma((15,)), dma((15,))],
            compiler_params=pltpu.CompilerParams(collective_id=0, has_side_effects=True),
            cost_estimate=cost(8_000_000_000, 2_000_000), name='dispatch',
        )(x_loc, meta, send)

        me = lax.axis_index('ep')
        owner = mig_src // slots
        i_own = (owner[0] == me) | (owner[1] == me)
        chip_own = (owner[0] // 2 == me // 2) | (owner[1] // 2 == me // 2)
        part = half // 2
        held0 = jnp.where(i_own, own[:part], near[:part])
        held1 = jnp.where(i_own, own[part:], near[part:])
        rx1 = lax.ppermute(held0, 'ep', to_x)
        ry1 = lax.ppermute(held1, 'ep', to_y)

        buf = [pltpu.VMEM((HALF, depth, width), BF16)] * 2 + [pltpu.VMEM((HALF, width, depth), BF16)]
        *new, xg, at, gr, c = pl.pallas_call(
            first_kernel,
            out_shape=shapes + (jax.ShapeDtypeStruct((later, model), BF16), jax.ShapeDtypeStruct((total, rows), BF16),
                                jax.ShapeDtypeStruct((later, 128), F32), jax.ShapeDtypeStruct((HALF * per, model), BF16)),
            in_specs=[SMEM] + [ANY] * 5, out_specs=(ANY,) * 7,
            scratch_shapes=buf + [
                pltpu.VMEM((total, model), BF16), pltpu.VMEM((groups, 16, 128), F32),
                pltpu.VMEM((rows, model), BF16), pltpu.VMEM((rows, total), BF16), pltpu.VMEM((total, rows), BF16),
                pltpu.VMEM((rows, 128), F32), pltpu.VMEM((HALF * per, model), BF16),
                pltpu.VMEM((slots, total), F32), pltpu.VMEM((slots, total), F32), pltpu.VMEM((16, total), F32),
                dma((3, HALF)), dma((3, HALF)), dma((4,))],
            compiler_params=pltpu.CompilerParams(vmem_limit_bytes=LIMIT),
            cost_estimate=cost(40_000_000_000, 2 * HALF * slot_bytes), name='first',
        )(old_map, xall.reshape(total, model), mall, *weights)

        rx1, ry1, xg = lax.optimization_barrier((rx1, ry1, xg))
        next_x = jnp.where(chip_own, held1, ry1)
        next_y = jnp.where(chip_own, held0, rx1)
        next_x, next_y, xg = lax.optimization_barrier((next_x, next_y, xg))
        rx2 = lax.ppermute(next_x, 'ep', to_x)
        ry2 = lax.ppermute(next_y, 'ep', to_y)

        *new, psum = pl.pallas_call(
            second_kernel,
            out_shape=shapes + (jax.ShapeDtypeStruct((total, model), F32),),
            in_specs=[ANY] * 10, out_specs=(ANY,) * 4,
            input_output_aliases={7: 0, 8: 1, 9: 2},
            scratch_shapes=buf + [
                pltpu.VMEM((later, model), BF16), pltpu.VMEM((total, rows), BF16), pltpu.VMEM((later, 128), F32),
                pltpu.VMEM((rows, model), BF16), pltpu.VMEM((total, model), F32),
                dma((3, HALF)), dma((3, HALF)), dma((4,))],
            compiler_params=pltpu.CompilerParams(vmem_limit_bytes=LIMIT),
            cost_estimate=cost(40_000_000_000, 2 * HALF * slot_bytes), name='second',
        )(xg, at, gr, c, *weights, *new)

        y_out, got, gown = pl.pallas_call(
            combine_kernel,
            out_shape=(jax.ShapeDtypeStruct((tok, model), BF16), jax.ShapeDtypeStruct((4, part, width), BF16),
                       jax.ShapeDtypeStruct((half, width), BF16)),
            in_specs=[ANY, VMEM] + [ANY] * 5, out_specs=(VMEM, ANY, ANY),
            scratch_shapes=[pltpu.VMEM((4, tok, model), F32), pltpu.VMEM((4, tok, model), F32),
                            pltpu.VMEM((4, tok, model), F32), pltpu.VMEM((3, tok, model), F32),
                            dma((4,)), dma((12,)), dma((12,))],
            compiler_params=pltpu.CompilerParams(collective_id=1, has_side_effects=True),
            cost_estimate=cost(16_000_000_000, 4_000_000), name='combine',
        )(psum.reshape(groups, tok, model), x_loc, rx1, ry1, rx2, ry2, own)

        new = pl.pallas_call(
            patch_kernel,
            out_shape=shapes,
            in_specs=[SMEM, SMEM] + [ANY] * 13, out_specs=(ANY, ANY, ANY),
            input_output_aliases={12: 0, 13: 1, 14: 2},
            scratch_shapes=[pltpu.VMEM((3 * depth, width), BF16), dma((5,))],
            cost_estimate=cost(3_000_000_000, 2 * slot_bytes), name='patch',
        )(mig_src, mig_dst, rx1, ry1, rx2, ry2, got, near, gown, *weights, *new)
        return (y_out, *new)

    row_spec = P(('dp', 'ep'), None)
    slot_spec = P('ep', None, None)
    return jax.shard_map(local_step, mesh=mesh, in_specs=(row_spec, row_spec, row_spec, slot_spec, slot_spec, slot_spec, P(), P(), P()), out_specs=(row_spec, slot_spec, slot_spec, slot_spec), check_vma=False)
```

```python
import jax
import jax.numpy as jnp
from jax import lax
from jax.experimental import pallas as pl
from jax.experimental.pallas import tpu as pltpu
from jax.sharding import PartitionSpec as P

MESH = pl.DeviceIdType.MESH
BF16, F32 = jnp.bfloat16, jnp.float32
ANY = pl.BlockSpec(memory_space=pl.ANY)
VMEM = pl.BlockSpec(memory_space=pltpu.VMEM)
SMEM = pl.BlockSpec(memory_space=pltpu.SMEM)
HBM = pl.BlockSpec(memory_space=pltpu.HBM)
MIB = 1024 * 1024
HALF = 8


def places():
    me = lax.axis_index('ep')
    core, chip = me % 2, me // 2
    x, y = chip % 2, chip // 2
    sib = chip * 2 + 1 - core
    chips = ((1 - y) * 2 + 1 - x, y * 2 + 1 - x, (1 - y) * 2 + x)
    return me, core, chip, sib, chips


def enter(partners):
    barrier = pltpu.get_barrier_semaphore()
    for dev in partners:
        pl.semaphore_signal(barrier, inc=1, device_id={'ep': dev}, device_id_type=MESH)
    pl.semaphore_wait(barrier, len(partners))


def remote(src, dst, send, recv, dev):
    return pltpu.make_async_remote_copy(src, dst, send, recv, device_id={'ep': dev}, device_id_type=MESH)


def pack_kernel(src, ids_ref, gate_ref, wg, wu, wd, meta_ref, flag_ref, send_ref, own_ref, sem):
    me = lax.axis_index('ep')
    slots, depth, width = wg.shape
    owner = [src[i] // slots for i in range(2)]
    flag_ref[0] = jnp.where((owner[0] == me) | (owner[1] == me), 1, 0)
    flag_ref[1] = jnp.where((owner[0] // 2 == me // 2) | (owner[1] // 2 == me // 2), 1, 0)
    tok = ids_ref.shape[1]
    meta_ref[...] = jnp.zeros_like(meta_ref)
    meta_ref[0:8, 0:tok] = ids_ref[...].astype(F32)
    meta_ref[8:16, 0:tok] = gate_ref[...]
    half = 3 * depth // 2
    slot = jnp.where(src[0] // slots == me, src[0], src[1]) % slots

    def first(ref, k):
        return [pltpu.make_async_copy(wg.at[slot], ref.at[pl.ds(0, depth)], sem.at[k]),
                pltpu.make_async_copy(wu.at[slot, pl.ds(0, half - depth)], ref.at[pl.ds(depth, half - depth)], sem.at[k + 1])]

    def second(ref, k):
        rest = 2 * depth - half
        copies = [pltpu.make_async_copy(wu.at[slot, pl.ds(half - depth, rest)], ref.at[pl.ds(0, rest)], sem.at[k])]
        for b in range(depth // width):
            copies.append(pltpu.make_async_copy(wd.at[slot, :, pl.ds(width * b, width)],
                                                ref.at[pl.ds(rest + width * b, width)], sem.at[k + 1 + b]))
        return copies

    def run(copies):
        for copy in copies:
            copy.start()
        for copy in copies:
            copy.wait()

    @pl.when(me % 2 == 0)
    def _():
        run(second(send_ref, 2) + first(own_ref, 0))

    @pl.when(me % 2 == 1)
    def _():
        run(first(send_ref, 0) + second(own_ref, 2))


def dispatch_kernel(x_ref, meta_ref, slot_ref, xall, mall, near, send, recv):
    me, core, chip, sib, chips = places()
    peers = [c * 2 + core for c in chips]
    enter(peers + [sib])

    def pair(k, src_x, src_m, block, dev):
        return (remote(src_x, xall.at[block], send.at[2 * k], recv.at[2 * k], dev),
                remote(src_m, mall.at[block], send.at[2 * k + 1], recv.at[2 * k + 1], dev))

    first = [pair(k, x_ref, meta_ref, me, peers[k]) for k in range(3)]
    first.append(pair(3, x_ref, meta_ref, me, sib))
    for group in first:
        for copy in group:
            copy.start()
    slot = remote(slot_ref, near, send.at[14], recv.at[14], sib)
    slot.start()
    xall[pl.ds(me, 1)] = x_ref[...][None]
    mall[pl.ds(me, 1)] = meta_ref[...][None]
    second = []
    for k in (1, 2, 0):
        for copy in first[k]:
            copy.wait_recv()
        fwd = pair(4 + k, xall.at[peers[k]], mall.at[peers[k]], peers[k], sib)
        for copy in fwd:
            copy.start()
        second.append(fwd)
    for copy in first[3]:
        copy.wait_recv()
    for group in first:
        for copy in group:
            copy.wait_send()
    for group in second:
        for copy in group:
            copy.wait()
    slot.wait()


def stream(slots0, count, w, w_new, bufs, sem_in, sem_out):
    def load(i):
        return [pltpu.make_async_copy(w[k].at[slots0 + i], bufs[k].at[i], sem_in.at[k, i]) for k in range(3)]

    def drain(i):
        return [pltpu.make_async_copy(bufs[k].at[i], w_new[k].at[slots0 + i], sem_out.at[k, i]) for k in range(3)]

    return load, drain


def experts(i, xs, gate, bufs):
    act_g = jnp.dot(xs, bufs[0][i], preferred_element_type=F32)
    act_u = jnp.dot(xs, bufs[1][i], preferred_element_type=F32)
    z = (jax.nn.silu(act_g) * act_u).astype(BF16)
    o = jnp.dot(z, bufs[2][i], preferred_element_type=F32)
    return (o * gate).astype(BF16)


def first_kernel(old_map, x_ref, mall, wg, wu, wd, wg_new, wu_new, wd_new, xg_out, at_ref, gr_out, c_ref,
                 bg, bu, bd, xg, a_ref, gr_ref, pos, gsc, meta, sem_in, sem_out):
    me = lax.axis_index('ep')
    slots, tok, cap = wg.shape[0], 64, 8
    total = x_ref.shape[0]
    devs = total // tok
    rows = devs * cap
    bufs = (bg, bu, bd)
    load, drain = stream(0, HALF, (wg, wu, wd), (wg_new, wu_new, wd_new), bufs, sem_in, sem_out)
    for i in range(HALF):
        for copy in load(i):
            copy.start()
    done = HALF * rows

    lane = lax.broadcasted_iota(jnp.int32, (16, 128), 1)
    for p in range(devs // 2):
        other = pltpu.roll(mall[2 * p + 1], 64, axis=1)
        meta[:, pl.ds(128 * p, 128)] = jnp.where(lane < 64, mall[2 * p], other)
    ids = meta[0:8, :]
    gates = meta[8:16, :]
    hits, gs = [], []
    for j in range(slots):
        same = ids == old_map[me * slots + j].astype(F32)
        hits.append(jnp.sum(jnp.where(same, 1.0, 0.0), axis=0, keepdims=True))
        gs.append(jnp.sum(jnp.where(same, gates, 0.0), axis=0, keepdims=True))
    hit = jnp.concatenate(hits, axis=0)
    gsc[...] = jnp.concatenate(gs, axis=0)
    t_row = lax.broadcasted_iota(jnp.int32, (total, total), 0)
    t_col = lax.broadcasted_iota(jnp.int32, (total, total), 1)
    before = jnp.where((t_row < t_col) & (t_row // tok == t_col // tok), 1.0, 0.0).astype(BF16)
    rank = jnp.dot(hit.astype(BF16), before, preferred_element_type=F32)
    owner = (lax.broadcasted_iota(jnp.int32, (slots, total), 1) // tok * cap).astype(F32)
    pos[...] = jnp.where(hit > 0.5, rank + owner, -1.0)
    post = jnp.transpose(jnp.concatenate([pos[...], jnp.full((128 - slots, total), -1.0, F32)], axis=0))
    wide = lax.broadcasted_iota(jnp.int32, (total, 128), 1)
    for p in range(slots // 2):
        want = jnp.where(wide < rows, post[:, 2 * p:2 * p + 1], post[:, 2 * p + 1:2 * p + 2])
        at_ref[:, pl.ds(128 * p, 128)] = jnp.where(want == (wide % rows).astype(F32), 1.0, 0.0).astype(BF16)

    row_id = lax.broadcasted_iota(jnp.int32, (rows, total), 0).astype(F32)

    def choose(first, count, g_ref):
        @pl.loop(0, count)
        def _(j):
            chosen = row_id == pos[pl.ds(first + j, 1), :]
            a_ref[pl.ds(pl.multiple_of((first + j) * rows, rows), rows), :] = jnp.where(chosen, 1.0, 0.0).astype(BF16)
            g = jnp.sum(jnp.where(chosen, gsc[pl.ds(first + j, 1), :], 0.0), axis=1, keepdims=True)
            g_ref[pl.ds(pl.multiple_of(j * rows, rows), rows), :] = jnp.broadcast_to(g, (rows, 128))

    def gather(first, count, to_ref):
        @pl.loop(0, count // (4 * rows))
        def _(q):
            r0 = pl.multiple_of(q * 4 * rows, 4 * rows)
            picked = jnp.dot(a_ref[pl.ds(first + r0, 4 * rows), :], x_ref[...], preferred_element_type=F32)
            to_ref[pl.ds(r0, 4 * rows), :] = picked.astype(BF16)

    choose(0, HALF, gr_ref)
    gather(0, done, xg)

    @pl.loop(0, HALF)
    def _(i):
        for copy in load(i):
            copy.wait()
        for copy in drain(i):
            copy.start()
        r0 = pl.multiple_of(i * rows, rows)
        c_ref[pl.ds(r0, rows), :] = experts(i, xg[pl.ds(r0, rows), :], gr_ref[pl.ds(r0, rows), 0:1], bufs)

    choose(HALF, slots - HALF, gr_out)
    gather(done, (slots - HALF) * rows, xg_out)
    for i in range(HALF):
        for copy in drain(i):
            copy.wait()


def second_kernel(xg, at_ref, gr_ref, c_early, wg, wu, wd, wg_old, wu_old, wd_old, wg_new, wu_new, wd_new, out_ref,
                  bg, bu, bd, c_ref, sem_in, sem_out):
    slots = wg.shape[0]
    count = slots - HALF
    rows = xg.shape[0] // count
    bufs = (bg, bu, bd)
    load, drain = stream(HALF, count, (wg, wu, wd), (wg_new, wu_new, wd_new), bufs, sem_in, sem_out)
    for i in range(count):
        for copy in load(i):
            copy.start()

    @pl.loop(0, count)
    def _(i):
        for copy in load(i):
            copy.wait()
        for copy in drain(i):
            copy.start()
        r0 = pl.multiple_of(i * rows, rows)
        c_ref[pl.ds(r0, rows), :] = experts(i, xg[pl.ds(r0, rows), :], gr_ref[pl.ds(r0, rows), 0:1], bufs)

    cols = 256
    done = HALF * rows

    @pl.loop(0, out_ref.shape[1] // cols)
    def _(n):
        at = pl.ds(pl.multiple_of(n * cols, cols), cols)
        out_ref[:, at] = (jnp.dot(at_ref[:, 0:done], c_early[:, at], preferred_element_type=F32)
                          + jnp.dot(at_ref[:, done:], c_ref[:, at], preferred_element_type=F32))

    for i in range(count):
        for copy in drain(i):
            copy.wait()


def combine_kernel(part, x_ref, rx1, ry1, rx2, ry2, own, y_ref, got, gown, near, summed, far, send, recv):
    me, core, chip, sib, chips = places()
    peers = [c * 2 + core for c in chips]
    order = list(chips) + [chip]
    enter(peers + [sib])
    across = [remote(part.at[c * 2 + 1 - core], near.at[k], send.at[k], recv.at[k], sib) for k, c in enumerate(order)]
    for copy in across:
        copy.start()
    out = [remote(summed.at[k], far.at[k], send.at[4 + k], recv.at[4 + k], peers[k]) for k in range(3)]
    moved = [remote(r, got.at[k], send.at[7 + k], recv.at[7 + k], sib) for k, r in enumerate((rx1, ry1, rx2, ry2))]
    moved.append(remote(own, gown, send.at[11], recv.at[11], sib))
    for copy in moved:
        copy.start()
    for k in range(4):
        across[k].wait_recv()
        summed[k] = part[order[k] * 2 + core] + near[k]
        if k >= 1:
            out[k - 1].start()
    acc = x_ref[...].astype(F32) + summed[3]
    for k in (1, 2, 0):
        out[k].wait_recv()
        acc = acc + far[k]
    y_ref[...] = acc.astype(BF16)
    for copy in moved:
        copy.wait_recv()
    for copy in across + out + moved:
        copy.wait_send()


def patch_kernel(src, dst, rx1, ry1, rx2, ry2, got, near, gown, wg, wu, wd, wg_old, wu_old, wd_old,
                 wg_new, wu_new, wd_new, buf, sem):
    me = lax.axis_index('ep')
    core = me % 2
    slots, depth, width = wg.shape
    part = rx1.shape[0]
    owner = [dst[i] // slots for i in range(2)]
    here = [owner[i] == me for i in range(2)]
    chip = [owner[i] // 2 for i in range(2)]
    local = here[0] & here[1]
    comes = (here[0] | here[1]) & jnp.logical_not(local)
    same_x, same_y = chip[0] % 2 == chip[1] % 2, chip[0] // 2 == chip[1] // 2

    def quarters(slot):
        rest = 2 * part - depth
        return ([(0, part, wg_new, 0, None)],
                [(0, depth - part, wg_new, part, None), (depth - part, rest, wu_new, 0, None)],
                [(0, depth - rest, wu_new, rest, None), (depth - rest, part - depth + rest, wd_new, 0, 0)],
                [(0, width - (part - depth + rest), wd_new, part - depth + rest, 0)]
                + [(width - (part - depth + rest) + width * b, width, wd_new, 0, b + 1) for b in range(2)])

    def put(refs, slot):
        copies = []
        for ref, pieces in zip(refs, quarters(slot)):
            for r0, n, new, to, b in pieces:
                where = new.at[slot, pl.ds(to, n)] if b is None else new.at[slot, pl.ds(to, n), pl.ds(width * b, width)]
                copies.append(pltpu.make_async_copy(ref.at[pl.ds(r0, n)], where, sem.at[len(copies)]))
        for copy in copies:
            copy.start()
        for copy in copies:
            copy.wait()

    def receive(case, a0, a1, b0, b1):
        for c in range(2):
            @pl.when(comes & case & (core == c))
            def _(refs=(a0, a1, b0, b1) if c == 0 else (b0, b1, a0, a1)):
                put(refs, jnp.where(here[0], dst[0], dst[1]) % slots)

    other = jnp.logical_not
    rows = pl.ds(0, part), pl.ds(part, part)
    receive(same_y & same_x, near.at[rows[0]], near.at[rows[1]], gown.at[rows[0]], gown.at[rows[1]])
    receive(same_y & other(same_x), rx1, rx2, got.at[0], got.at[2])
    receive(same_x & other(same_y), ry2, ry1, got.at[3], got.at[1])
    receive(other(same_x) & other(same_y), ry2, rx2, got.at[3], got.at[2])

    @pl.when(local)
    def _():
        for i in range(2):
            s = src[i] % slots
            copies = [pltpu.make_async_copy(wg.at[s], buf.at[pl.ds(0, depth)], sem.at[0]),
                      pltpu.make_async_copy(wu.at[s], buf.at[pl.ds(depth, depth)], sem.at[1])]
            for b in range(depth // width):
                copies.append(pltpu.make_async_copy(wd.at[s, :, pl.ds(width * b, width)],
                                                    buf.at[pl.ds(2 * depth + width * b, width)], sem.at[2 + b]))
            for copy in copies:
                copy.start()
            for copy in copies:
                copy.wait()
            put([buf.at[pl.ds(part * k, part)] for k in range(4)], dst[i] % slots)


def cost(flops, moved):
    return pl.CostEstimate(flops=flops, bytes_accessed=moved, transcendentals=0)


def solution(mesh):
    groups = mesh.shape['ep']

    def flip(bit):
        return [(d, d + bit - 2 * bit * ((d // bit) % 2)) for d in range(groups)]

    to_x, to_y = flip(2), flip(4)

    def local_step(x_loc, expert_ids, gate_val, w_gate, w_up, w_down, old_map, mig_src, mig_dst):
        tok, model = x_loc.shape
        slots, depth, width = w_gate.shape
        total = groups * tok
        per = groups * 8
        rows = slots * per
        later = (slots - HALF) * per
        half = 3 * depth // 2
        weights = (w_gate, w_up, w_down)
        shapes = tuple(jax.ShapeDtypeStruct(w.shape, BF16) for w in weights)
        dma = pltpu.SemaphoreType.DMA
        slot_bytes = 6 * depth * width

        meta, flags, send, own = pl.pallas_call(
            pack_kernel,
            out_shape=(jax.ShapeDtypeStruct((16, 128), F32), jax.ShapeDtypeStruct((2,), jnp.int32))
            + (jax.ShapeDtypeStruct((half, width), BF16),) * 2,
            in_specs=[SMEM, VMEM, VMEM, HBM, HBM, HBM], out_specs=(VMEM, SMEM, VMEM, VMEM),
            scratch_shapes=[dma((6,))],
            compiler_params=pltpu.CompilerParams(vmem_limit_bytes=42 * MIB),
            cost_estimate=cost(2_000_000_000, 2 * slot_bytes), name='pack',
        )(mig_src, expert_ids.T, gate_val.T, *weights)

        xall, mall, near = pl.pallas_call(
            dispatch_kernel,
            out_shape=(jax.ShapeDtypeStruct((groups, tok, model), BF16), jax.ShapeDtypeStruct((groups, 16, 128), F32),
                       jax.ShapeDtypeStruct((half, width), BF16)),
            in_specs=[VMEM, VMEM, ANY], out_specs=(VMEM, VMEM, ANY),
            scratch_shapes=[dma((15,)), dma((15,))],
            compiler_params=pltpu.CompilerParams(collective_id=0, has_side_effects=True, vmem_limit_bytes=8 * MIB),
            cost_estimate=cost(8_000_000_000, 2_000_000), name='dispatch',
        )(x_loc, meta, send)

        i_own, chip_own = flags[0] > 0, flags[1] > 0
        part = half // 2
        held0 = jnp.where(i_own, own[:part], near[:part])
        held1 = jnp.where(i_own, own[part:], near[part:])
        rx1 = lax.ppermute(held0, 'ep', to_x)
        ry1 = lax.ppermute(held1, 'ep', to_y)

        buf = [pltpu.VMEM((HALF, depth, width), BF16)] * 2 + [pltpu.VMEM((HALF, width, depth), BF16)]
        *new, xg, at, gr, c = pl.pallas_call(
            first_kernel,
            out_shape=shapes + (jax.ShapeDtypeStruct((later, model), BF16), jax.ShapeDtypeStruct((total, rows), BF16),
                                jax.ShapeDtypeStruct((later, 128), F32), jax.ShapeDtypeStruct((HALF * per, model), BF16)),
            in_specs=[SMEM, VMEM, VMEM, HBM, HBM, HBM], out_specs=(HBM,) * 3 + (VMEM,) * 4,
            scratch_shapes=buf + [
                pltpu.VMEM((HALF * per, model), BF16), pltpu.VMEM((rows, total), BF16), pltpu.VMEM((HALF * per, 128), F32),
                pltpu.VMEM((slots, total), F32), pltpu.VMEM((slots, total), F32), pltpu.VMEM((16, total), F32),
                dma((3, HALF)), dma((3, HALF))],
            compiler_params=pltpu.CompilerParams(vmem_limit_bytes=42 * MIB),
            cost_estimate=cost(40_000_000_000, 2 * HALF * slot_bytes), name='first',
        )(old_map, xall.reshape(total, model), mall, *weights)

        rx1, ry1, xg = lax.optimization_barrier((rx1, ry1, xg))
        next_x = jnp.where(chip_own, held1, ry1)
        next_y = jnp.where(chip_own, held0, rx1)
        next_x, next_y, xg = lax.optimization_barrier((next_x, next_y, xg))
        rx2 = lax.ppermute(next_x, 'ep', to_x)
        ry2 = lax.ppermute(next_y, 'ep', to_y)

        *new, psum = pl.pallas_call(
            second_kernel,
            out_shape=shapes + (jax.ShapeDtypeStruct((total, model), F32),),
            in_specs=[VMEM] * 4 + [HBM] * 6, out_specs=(HBM,) * 3 + (VMEM,),
            input_output_aliases={7: 0, 8: 1, 9: 2},
            scratch_shapes=buf + [
                pltpu.VMEM((later, model), BF16), dma((3, HALF)), dma((3, HALF))],
            compiler_params=pltpu.CompilerParams(vmem_limit_bytes=42 * MIB),
            cost_estimate=cost(40_000_000_000, 2 * HALF * slot_bytes), name='second',
        )(xg, at, gr, c, *weights, *new)

        y_out, got, gown = pl.pallas_call(
            combine_kernel,
            out_shape=(jax.ShapeDtypeStruct((tok, model), BF16), jax.ShapeDtypeStruct((4, part, width), BF16),
                       jax.ShapeDtypeStruct((half, width), BF16)),
            in_specs=[VMEM, VMEM] + [ANY] * 5, out_specs=(VMEM, ANY, ANY),
            scratch_shapes=[pltpu.VMEM((4, tok, model), F32), pltpu.VMEM((4, tok, model), F32),
                            pltpu.VMEM((3, tok, model), F32), dma((12,)), dma((12,))],
            compiler_params=pltpu.CompilerParams(collective_id=1, has_side_effects=True, vmem_limit_bytes=24 * MIB),
            cost_estimate=cost(16_000_000_000, 4_000_000), name='combine',
        )(psum.reshape(groups, tok, model), x_loc, rx1, ry1, rx2, ry2, own)

        new = pl.pallas_call(
            patch_kernel,
            out_shape=shapes,
            in_specs=[SMEM, SMEM] + [VMEM] * 7 + [HBM] * 6, out_specs=(HBM,) * 3,
            input_output_aliases={12: 0, 13: 1, 14: 2},
            scratch_shapes=[pltpu.VMEM((3 * depth, width), BF16), dma((9,))],
            compiler_params=pltpu.CompilerParams(vmem_limit_bytes=40 * MIB),
            cost_estimate=cost(3_000_000_000, 2 * slot_bytes), name='patch',
        )(mig_src, mig_dst, rx1, ry1, rx2, ry2, got, near, gown, *weights, *new)
        return (y_out, *new)

    row_spec = P(('dp', 'ep'), None)
    slot_spec = P('ep', None, None)
    return jax.shard_map(local_step, mesh=mesh, in_specs=(row_spec, row_spec, row_spec, slot_spec, slot_spec, slot_spec, P(), P(), P()), out_specs=(row_spec, slot_spec, slot_spec, slot_spec), check_vma=False)
```

```python
import jax
import jax.numpy as jnp
from jax import lax
from jax.experimental import pallas as pl
from jax.experimental.pallas import tpu as pltpu
from jax.sharding import PartitionSpec as P

MESH = pl.DeviceIdType.MESH
BF16, F32 = jnp.bfloat16, jnp.float32
ANY = pl.BlockSpec(memory_space=pl.ANY)
VMEM = pl.BlockSpec(memory_space=pltpu.VMEM)
SMEM = pl.BlockSpec(memory_space=pltpu.SMEM)
HBM = pl.BlockSpec(memory_space=pltpu.HBM)
MIB = 1024 * 1024
HELD = 2
EARLY, SECOND, THIRD = 6, 4, 4
FIRST = EARLY + 2


def places():
    me = lax.axis_index('ep')
    core, chip = me % 2, me // 2
    x, y = chip % 2, chip // 2
    sib = chip * 2 + 1 - core
    chips = ((1 - y) * 2 + 1 - x, y * 2 + 1 - x, (1 - y) * 2 + x)
    return me, core, chip, sib, chips


def enter(partners):
    barrier = pltpu.get_barrier_semaphore()
    for dev in partners:
        pl.semaphore_signal(barrier, inc=1, device_id={'ep': dev}, device_id_type=MESH)
    pl.semaphore_wait(barrier, len(partners))


def remote(src, dst, send, recv, dev):
    return pltpu.make_async_remote_copy(src, dst, send, recv, device_id={'ep': dev}, device_id_type=MESH)


def pack_kernel(src, ids_ref, gate_ref, wg, wu, wd, meta_ref, mine_ref, chip_ref, send_ref, own_ref, sem):
    me = lax.axis_index('ep')
    slots, depth, width = wg.shape
    owner = [src[i] // slots for i in range(2)]
    mine_ref[0] = jnp.where((owner[0] == me) | (owner[1] == me), 1, 0)
    chip_ref[0] = jnp.where((owner[0] // 2 == me // 2) | (owner[1] // 2 == me // 2), 1, 0)
    tok = ids_ref.shape[1]
    meta_ref[...] = jnp.zeros_like(meta_ref)
    meta_ref[0:8, 0:tok] = ids_ref[...].astype(F32)
    meta_ref[8:16, 0:tok] = gate_ref[...]
    half = 3 * depth // 2
    slot = jnp.where(src[0] // slots == me, src[0], src[1]) % slots

    def first(ref, k):
        return [pltpu.make_async_copy(wg.at[slot], ref.at[pl.ds(0, depth)], sem.at[k]),
                pltpu.make_async_copy(wu.at[slot, pl.ds(0, half - depth)], ref.at[pl.ds(depth, half - depth)], sem.at[k + 1])]

    def second(ref, k):
        rest = 2 * depth - half
        copies = [pltpu.make_async_copy(wu.at[slot, pl.ds(half - depth, rest)], ref.at[pl.ds(0, rest)], sem.at[k])]
        for b in range(depth // width):
            copies.append(pltpu.make_async_copy(wd.at[slot, :, pl.ds(width * b, width)],
                                                ref.at[pl.ds(rest + width * b, width)], sem.at[k + 1 + b]))
        return copies

    def run(copies):
        for copy in copies:
            copy.start()
        for copy in copies:
            copy.wait()

    @pl.when(me % 2 == 0)
    def _():
        run(second(send_ref, 2) + first(own_ref, 0))

    @pl.when(me % 2 == 1)
    def _():
        run(first(send_ref, 0) + second(own_ref, 2))


def dispatch_kernel(mine_ref, x_ref, meta_ref, slot_ref, own, wg, wu, wd, xall, mall, near, h0, h1, h2, h3, *rest):
    me, core, chip, sib, chips = places()
    peers = [c * 2 + core for c in chips]
    bufs, (send, recv, sem) = rest[:-3], rest[-3:]
    per = len(bufs) // 3
    size = EARLY // per
    reads = [pltpu.make_async_copy(w.at[pl.ds(i * size, size)], bufs[k * per + i], sem.at[k * per + i])
             for i in range(per) for k, w in enumerate((wg, wu, wd))]
    for copy in reads:
        copy.start()
    enter(peers + [sib])

    def pair(k, src_x, src_m, block, dev):
        return (remote(src_x, xall.at[block], send.at[2 * k], recv.at[2 * k], dev),
                remote(src_m, mall.at[block], send.at[2 * k + 1], recv.at[2 * k + 1], dev))

    first = [pair(k, x_ref, meta_ref, me, peers[k]) for k in range(3)]
    first.append(pair(3, x_ref, meta_ref, me, sib))
    for group in first:
        for copy in group:
            copy.start()
    slot = remote(slot_ref, near, send.at[14], recv.at[14], sib)
    slot.start()
    xall[pl.ds(me, 1)] = x_ref[...][None]
    mall[pl.ds(me, 1)] = meta_ref[...][None]
    slot.wait_recv()
    part = h0.shape[0]
    for k, held in enumerate((h0, h1, h2, h3)):
        rows = pl.ds(k * part, part)
        held[...] = jnp.where(mine_ref[0] > 0, own[rows, :], near[rows, :])
    second = []
    for k in (1, 2, 0):
        for copy in first[k]:
            copy.wait_recv()
        fwd = pair(4 + k, xall.at[peers[k]], mall.at[peers[k]], peers[k], sib)
        for copy in fwd:
            copy.start()
        second.append(fwd)
    for copy in first[3]:
        copy.wait_recv()
    for group in first:
        for copy in group:
            copy.wait_send()
    for group in second:
        for copy in group:
            copy.wait()
    slot.wait_send()
    for copy in reads:
        copy.wait()


def stream(slots0, count, w, w_new, bufs, sem_in, sem_out):
    def load(i):
        return [pltpu.make_async_copy(w[k].at[slots0 + i], bufs[k].at[i], sem_in.at[k, i]) for k in range(3)]

    def drain(i):
        return [pltpu.make_async_copy(bufs[k].at[i], w_new[k].at[slots0 + i], sem_out.at[k, i]) for k in range(3)]

    return load, drain


def experts(i, xs, gate, bufs):
    act_g = jnp.dot(xs, bufs[0][i], preferred_element_type=F32)
    act_u = jnp.dot(xs, bufs[1][i], preferred_element_type=F32)
    z = (jax.nn.silu(act_g) * act_u).astype(BF16)
    o = jnp.dot(z, bufs[2][i], preferred_element_type=F32)
    return (o * gate).astype(BF16)


def first_kernel(old_map, x_ref, mall, *rest):
    bufs, rest = rest[:-22], rest[-22:]
    wg, wu, wd, wg_new, wu_new, wd_new, xg_out, at_ref, gr_out, c_ref, eg, eu, ed, xg, a_ref, gr_ref, pos, gsc, meta = rest[:19]
    more_in, more_out, sem_out = rest[19:]
    me = lax.axis_index('ep')
    slots, tok, cap = wg_new.shape[0], 64, 8
    total = x_ref.shape[0]
    devs = total // tok
    rows = devs * cap
    done = FIRST * rows
    more = (eg, eu, ed)
    load, drain = stream(EARLY, FIRST - EARLY, (wg, wu, wd), (wg_new, wu_new, wd_new), more, more_in, more_out)
    for i in range(FIRST - EARLY):
        for copy in load(i):
            copy.start()
    held = len(bufs) // 3
    size = EARLY // held
    drains = [pltpu.make_async_copy(bufs[k * held + i], new.at[pl.ds(i * size, size)], sem_out.at[k, i])
              for i in range(held) for k, new in enumerate((wg_new, wu_new, wd_new))]
    for copy in drains:
        copy.start()

    lane = lax.broadcasted_iota(jnp.int32, (16, 128), 1)
    for p in range(devs // 2):
        other = pltpu.roll(mall[2 * p + 1], 64, axis=1)
        meta[:, pl.ds(128 * p, 128)] = jnp.where(lane < 64, mall[2 * p], other)
    ids = meta[0:8, :]
    gates = meta[8:16, :]
    hits, gs = [], []
    for j in range(slots):
        same = ids == old_map[me * slots + j].astype(F32)
        hits.append(jnp.sum(jnp.where(same, 1.0, 0.0), axis=0, keepdims=True))
        gs.append(jnp.sum(jnp.where(same, gates, 0.0), axis=0, keepdims=True))
    hit = jnp.concatenate(hits, axis=0)
    gsc[...] = jnp.concatenate(gs, axis=0)
    t_row = lax.broadcasted_iota(jnp.int32, (total, total), 0)
    t_col = lax.broadcasted_iota(jnp.int32, (total, total), 1)
    before = jnp.where((t_row < t_col) & (t_row // tok == t_col // tok), 1.0, 0.0).astype(BF16)
    rank = jnp.dot(hit.astype(BF16), before, preferred_element_type=F32)
    owner = (lax.broadcasted_iota(jnp.int32, (slots, total), 1) // tok * cap).astype(F32)
    pos[...] = jnp.where(hit > 0.5, rank + owner, -1.0)
    post = jnp.transpose(jnp.concatenate([pos[...], jnp.full((128 - slots, total), -1.0, F32)], axis=0))
    wide = lax.broadcasted_iota(jnp.int32, (total, 128), 1)
    for p in range(slots // 2):
        want = jnp.where(wide < rows, post[:, 2 * p:2 * p + 1], post[:, 2 * p + 1:2 * p + 2])
        at_ref[:, pl.ds(128 * p, 128)] = jnp.where(want == (wide % rows).astype(F32), 1.0, 0.0).astype(BF16)

    row_id = lax.broadcasted_iota(jnp.int32, (rows, total), 0).astype(F32)

    def choose(first, count, g_ref):
        @pl.loop(0, count)
        def _(j):
            chosen = row_id == pos[pl.ds(first + j, 1), :]
            a_ref[pl.ds(pl.multiple_of((first + j) * rows, rows), rows), :] = jnp.where(chosen, 1.0, 0.0).astype(BF16)
            g = jnp.sum(jnp.where(chosen, gsc[pl.ds(first + j, 1), :], 0.0), axis=1, keepdims=True)
            g_ref[pl.ds(pl.multiple_of(j * rows, rows), rows), :] = jnp.broadcast_to(g, (rows, 128))

    def gather(first, count, to_ref):
        step = max(d for d in range(16, 257, 16) if count % d == 0)

        @pl.loop(0, count // step)
        def _(q):
            r0 = pl.multiple_of(q * step, step)
            picked = jnp.dot(a_ref[pl.ds(first + r0, step), :], x_ref[...], preferred_element_type=F32)
            to_ref[pl.ds(r0, step), :] = picked.astype(BF16)

    choose(0, FIRST, gr_ref)
    gather(0, done, xg)

    for n in range(held):
        @pl.loop(0, size)
        def _(i):
            at = pl.ds(pl.multiple_of((n * size + i) * rows, rows), rows)
            c_ref[at, :] = experts(i, xg[at, :], gr_ref[at, 0:1], bufs[n::held])

    @pl.loop(0, FIRST - EARLY)
    def _(i):
        for copy in load(i):
            copy.wait()
        for copy in drain(i):
            copy.start()
        at = pl.ds(pl.multiple_of((EARLY + i) * rows, rows), rows)
        c_ref[at, :] = experts(i, xg[at, :], gr_ref[at, 0:1], more)

    choose(FIRST, slots - FIRST, gr_out)
    gather(done, (slots - FIRST) * rows, xg_out)
    for copy in drains:
        copy.wait()
    for i in range(FIRST - EARLY):
        for copy in drain(i):
            copy.wait()


def later(first_slot, xg, gr_ref, w, w_new, c_ref, c_base, bufs, sem_in, sem_out, finish):
    count = bufs[0].shape[0]
    rows = gr_ref.shape[0] // (w[0].shape[0] - FIRST)
    load, drain = stream(first_slot, count, w, w_new, bufs, sem_in, sem_out)
    for i in range(count):
        for copy in load(i):
            copy.start()
    base = (first_slot - FIRST) * rows

    @pl.loop(0, count)
    def _(i):
        for copy in load(i):
            copy.wait()
        for copy in drain(i):
            copy.start()
        r0 = pl.multiple_of(i * rows, rows)
        at = pl.ds(pl.multiple_of(base + r0, rows), rows)
        c_ref[pl.ds(pl.multiple_of(c_base + r0, rows), rows), :] = experts(i, xg[at, :], gr_ref[at, 0:1], bufs)

    finish()
    for i in range(count):
        for copy in drain(i):
            copy.wait()


def second_kernel(xg, gr_ref, wg, wu, wd, wg_old, wu_old, wd_old, wg_new, wu_new, wd_new, c_ref,
                  bg, bu, bd, sem_in, sem_out):
    later(FIRST, xg, gr_ref, (wg, wu, wd), (wg_new, wu_new, wd_new), c_ref, 0, (bg, bu, bd), sem_in, sem_out,
          lambda: None)


def third_kernel(xg, gr_ref, at_ref, c0, c1, wg, wu, wd, wg_old, wu_old, wd_old, wg_new, wu_new, wd_new, out_ref,
                 bg, bu, bd, c_ref, sem_in, sem_out):
    cols = 256
    n0 = c0.shape[0]
    done = n0 + c1.shape[0]

    def finish():
        c_ref[0:n0, :] = c0[...]
        c_ref[n0:done, :] = c1[...]

        @pl.loop(0, out_ref.shape[1] // cols)
        def _(n):
            at = pl.ds(pl.multiple_of(n * cols, cols), cols)
            out_ref[:, at] = jnp.dot(at_ref[...], c_ref[:, at], preferred_element_type=F32)

    later(FIRST + SECOND, xg, gr_ref, (wg, wu, wd), (wg_new, wu_new, wd_new), c_ref, done, (bg, bu, bd), sem_in, sem_out,
          finish)


def combine_kernel(part, x_ref, rx1, rx2, rx3, ry1, ry2, ry3, own, y_ref, got, gown, near, summed, far, relay, last,
                   send, recv):
    me, core, chip, sib, chips = places()
    dev_x, dev_y = chips[1] * 2 + core, chips[2] * 2 + core
    order = list(chips) + [chip]
    enter([dev_x, dev_y, sib])
    across = [remote(part.at[c * 2 + 1 - core], near.at[k], send.at[k], recv.at[k], sib) for k, c in enumerate(order)]
    for copy in across:
        copy.start()
    moved = [remote(r, got.at[k], send.at[10 + k], recv.at[10 + k], sib) for k, r in enumerate((rx1, rx2, rx3, ry1, ry2, ry3))]
    moved.append(remote(own, gown, send.at[16], recv.at[16], sib))
    for copy in moved:
        copy.start()
    half = x_ref.shape[1] // 2
    cols = (pl.ds(0, half), pl.ds(half, half))
    towards = (dev_x, dev_y)
    diag = [remote(summed.at[0, :, cols[h]], far.at[0, :, cols[h]], send.at[4 + h], recv.at[4 + h], towards[h]) for h in range(2)]
    next_ = [remote(summed.at[1 + h, :, cols[h]], far.at[1, :, cols[h]], send.at[6 + h], recv.at[6 + h], towards[h]) for h in range(2)]
    onward = [remote(relay.at[h], last.at[h], send.at[8 + h], recv.at[8 + h], towards[1 - h]) for h in range(2)]
    for k in range(4):
        across[k].wait_recv()
        summed[k] = part[order[k] * 2 + core] + near[k]
        if k == 1:
            for copy in diag:
                copy.start()
        elif k == 2:
            next_[0].start()
        elif k == 3:
            next_[1].start()
    acc = x_ref[...].astype(F32) + summed[3]
    for h in range(2):
        diag[h].wait_recv()
        relay[h] = summed[2 - h, :, cols[h]] + far[0, :, cols[h]]
    for h in range(2):
        onward[h].start()
    for h in range(2):
        next_[h].wait_recv()
    acc = acc + far[1]
    for h in range(2):
        onward[h].wait_recv()
        y_ref[:, cols[h]] = (acc[:, h * half:(h + 1) * half] + last[h]).astype(BF16)
    for copy in moved:
        copy.wait_recv()
    for copy in across + diag + next_ + onward + moved:
        copy.wait_send()


def patch_kernel(src, dst, rx1, rx2, rx3, ry1, ry2, ry3, got, near, gown, wg, wu, wd, wg_old, wu_old, wd_old,
                 wg_new, wu_new, wd_new, buf, sem):
    me = lax.axis_index('ep')
    core = me % 2
    slots, depth, width = wg.shape
    part = rx1.shape[0]
    count = 3 * depth // part
    owner = [dst[i] // slots for i in range(2)]
    here = [owner[i] == me for i in range(2)]
    chip = [owner[i] // 2 for i in range(2)]
    local = here[0] & here[1]
    comes = (here[0] | here[1]) & jnp.logical_not(local)
    same_x, same_y = chip[0] % 2 == chip[1] % 2, chip[0] // 2 == chip[1] // 2

    def put(refs, slot):
        spans = [(0, depth, wg_new, None), (depth, 2 * depth, wu_new, None)]
        spans += [(2 * depth + width * b, 2 * depth + width * (b + 1), wd_new, b) for b in range(depth // width)]
        copies, at = [], 0
        for ref in refs:
            n = ref.shape[0]
            for lo, hi, new, b in spans:
                r0, r1 = max(at, lo), min(at + n, hi)
                if r0 < r1:
                    rows = pl.ds(r0 - lo, r1 - r0)
                    where = new.at[slot, rows] if b is None else new.at[slot, rows, pl.ds(width * b, width)]
                    copies.append(pltpu.make_async_copy(ref.at[pl.ds(r0 - at, r1 - r0)], where, sem.at[len(copies)]))
            at += n
        for copy in copies:
            copy.start()
        for copy in copies:
            copy.wait()

    def receive(case, mine, theirs):
        for c in range(2):
            @pl.when(comes & case & (core == c))
            def _(refs=mine + theirs if c == 0 else theirs + mine):
                put(refs, jnp.where(here[0], dst[0], dst[1]) % slots)

    no = jnp.logical_not
    came = (rx1, rx2, rx3, ry1, ry2, ry3)
    for case, order in ((same_y & no(same_x), (0, 1, 2, 5)), (same_x & no(same_y), (2, 5, 4, 3)),
                        (no(same_x) & no(same_y), (4, 5, 2, 1))):
        receive(case, [came[k] for k in order], [got.at[k] for k in order])
    receive(same_y & same_x, [near], [gown])

    @pl.when(local)
    def _():
        for i in range(2):
            s = src[i] % slots
            copies = [pltpu.make_async_copy(wg.at[s], buf.at[pl.ds(0, depth)], sem.at[0]),
                      pltpu.make_async_copy(wu.at[s], buf.at[pl.ds(depth, depth)], sem.at[1])]
            for b in range(depth // width):
                copies.append(pltpu.make_async_copy(wd.at[s, :, pl.ds(width * b, width)],
                                                    buf.at[pl.ds(2 * depth + width * b, width)], sem.at[2 + b]))
            for copy in copies:
                copy.start()
            for copy in copies:
                copy.wait()
            put([buf], dst[i] % slots)


def cost(flops, moved):
    return pl.CostEstimate(flops=flops, bytes_accessed=moved, transcendentals=0)


def solution(mesh):
    groups = mesh.shape['ep']

    def flip(bit):
        return [(d, d + bit - 2 * bit * ((d // bit) % 2)) for d in range(groups)]

    to_x, to_y = flip(2), flip(4)

    def local_step(x_loc, expert_ids, gate_val, w_gate, w_up, w_down, old_map, mig_src, mig_dst):
        tok, model = x_loc.shape
        slots, depth, width = w_gate.shape
        total = groups * tok
        per = groups * 8
        rows = slots * per
        late = (slots - FIRST) * per
        half = 3 * depth // 2
        weights = (w_gate, w_up, w_down)
        shapes = tuple(jax.ShapeDtypeStruct(w.shape, BF16) for w in weights)
        dma = pltpu.SemaphoreType.DMA
        slot_bytes = 6 * depth * width

        def params(mib, **kw):
            return pltpu.CompilerParams(vmem_limit_bytes=mib * MIB, **kw)

        def bf(*shape):
            return jax.ShapeDtypeStruct(shape, BF16)

        meta, i_own, chip_own, send, own = pl.pallas_call(
            pack_kernel,
            out_shape=(jax.ShapeDtypeStruct((16, 128), F32),) + (jax.ShapeDtypeStruct((1,), jnp.int32),) * 2 + (bf(half, width),) * 2,
            in_specs=[SMEM, VMEM, VMEM, HBM, HBM, HBM], out_specs=(VMEM, SMEM, SMEM, VMEM, VMEM),
            scratch_shapes=[dma((6,))], compiler_params=params(42),
            cost_estimate=cost(2_000_000_000, 2 * slot_bytes), name='pack',
        )(mig_src, expert_ids.T, gate_val.T, *weights)

        part = half // 4
        xall, mall, near, h0, h1, h2, h3, *bufs = pl.pallas_call(
            dispatch_kernel,
            out_shape=(bf(groups, tok, model), jax.ShapeDtypeStruct((groups, 16, 128), F32), bf(half, width))
            + (bf(part, width),) * 4 + tuple(bf(HELD, *w.shape[1:]) for w in weights for _ in range(EARLY // HELD)),
            in_specs=[SMEM, VMEM, VMEM, ANY, VMEM, HBM, HBM, HBM], out_specs=(VMEM,) * (7 + 3 * (EARLY // HELD)),
            scratch_shapes=[dma((15,)), dma((15,)), dma((3 * (EARLY // HELD),))],
            compiler_params=params(4, collective_id=0, has_side_effects=True),
            cost_estimate=cost(8_000_000_000, 2_000_000), name='dispatch',
        )(i_own, x_loc, meta, send, own, *weights)

        chip_own = chip_own[0] > 0
        held = (h0, h1, h2, h3)

        def hop(to_x_rows, to_y_rows):
            return lax.ppermute(to_x_rows, 'ep', to_x), lax.ppermute(to_y_rows, 'ep', to_y)

        def onward(k_x, k_y, from_x, from_y, ready):
            from_x, from_y, *ready = lax.optimization_barrier((from_x, from_y, *ready))
            rows_x, rows_y = jnp.where(chip_own, held[k_x], from_y), jnp.where(chip_own, held[k_y], from_x)
            rows_x, rows_y, *ready = lax.optimization_barrier((rows_x, rows_y, *ready))
            return from_x, from_y, *hop(rows_x, rows_y), ready

        rx1, ry1 = hop(held[0], held[3])

        def room(count):
            return [pltpu.VMEM((count,) + w.shape[1:], BF16) for w in weights]

        *new, xg, at, gr, c0 = pl.pallas_call(
            first_kernel,
            out_shape=shapes + (bf(late, model), bf(total, rows), jax.ShapeDtypeStruct((late, 128), F32), bf(FIRST * per, model)),
            in_specs=[SMEM] + [VMEM] * (2 + 3 * (EARLY // HELD)) + [HBM] * 3, out_specs=(HBM,) * 3 + (VMEM,) * 4,
            scratch_shapes=room(FIRST - EARLY) + [
                pltpu.VMEM((FIRST * per, model), BF16), pltpu.VMEM((rows, total), BF16), pltpu.VMEM((FIRST * per, 128), F32),
                pltpu.VMEM((slots, total), F32), pltpu.VMEM((slots, total), F32), pltpu.VMEM((16, total), F32),
                dma((3, FIRST - EARLY)), dma((3, FIRST - EARLY)), dma((3, EARLY // HELD))],
            compiler_params=params(16), cost_estimate=cost(30_000_000_000, (2 * FIRST - EARLY) * slot_bytes), name='first',
        )(old_map, xall.reshape(total, model), mall, *bufs, *weights)

        rx1, ry1, rx2, ry2, (xg, c0) = onward(1, 2, rx1, ry1, (xg, c0))
        *new, c1 = pl.pallas_call(
            second_kernel,
            out_shape=shapes + (bf(SECOND * per, model),),
            in_specs=[VMEM] * 2 + [HBM] * 6, out_specs=(HBM,) * 3 + (VMEM,),
            input_output_aliases={5: 0, 6: 1, 7: 2},
            scratch_shapes=room(SECOND) + [dma((3, SECOND))] * 2,
            compiler_params=params(40), cost_estimate=cost(30_000_000_000, 2 * SECOND * slot_bytes), name='second',
        )(xg, gr, *weights, *new)

        rx2, ry2, rx3, ry3, (xg, c1) = onward(2, 1, rx2, ry2, (xg, c1))
        *new, psum = pl.pallas_call(
            third_kernel,
            out_shape=shapes + (jax.ShapeDtypeStruct((total, model), F32),),
            in_specs=[VMEM] * 5 + [HBM] * 6, out_specs=(HBM,) * 3 + (VMEM,),
            input_output_aliases={8: 0, 9: 1, 10: 2},
            scratch_shapes=room(THIRD) + [pltpu.VMEM((rows, model), BF16)] + [dma((3, THIRD))] * 2,
            compiler_params=params(40), cost_estimate=cost(30_000_000_000, 2 * THIRD * slot_bytes), name='third',
        )(xg, gr, at, c0, c1, *weights, *new)

        came = (rx1, rx2, rx3, ry1, ry2, ry3)
        y_out, got, gown = pl.pallas_call(
            combine_kernel,
            out_shape=(bf(tok, model), bf(6, part, width), bf(half, width)),
            in_specs=[VMEM, VMEM] + [ANY] * 7, out_specs=(VMEM, ANY, ANY),
            scratch_shapes=[pltpu.VMEM((4, tok, model), F32), pltpu.VMEM((4, tok, model), F32),
                            pltpu.VMEM((2, tok, model), F32), pltpu.VMEM((2, tok, model // 2), F32),
                            pltpu.VMEM((2, tok, model // 2), F32), dma((17,)), dma((17,))],
            compiler_params=params(24, collective_id=1, has_side_effects=True),
            cost_estimate=cost(16_000_000_000, 4_000_000), name='combine',
        )(psum.reshape(groups, tok, model), x_loc, *came, own)

        new = pl.pallas_call(
            patch_kernel,
            out_shape=shapes,
            in_specs=[SMEM, SMEM] + [VMEM] * 9 + [HBM] * 6, out_specs=(HBM,) * 3,
            input_output_aliases={14: 0, 15: 1, 16: 2},
            scratch_shapes=[pltpu.VMEM((3 * depth, width), BF16), dma((13,))],
            compiler_params=params(40), cost_estimate=cost(3_000_000_000, 2 * slot_bytes), name='patch',
        )(mig_src, mig_dst, *came, got, near, gown, *weights, *new)
        return (y_out, *new)

    row_spec = P(('dp', 'ep'), None)
    slot_spec = P('ep', None, None)
    return jax.shard_map(local_step, mesh=mesh, in_specs=(row_spec, row_spec, row_spec, slot_spec, slot_spec, slot_spec, P(), P(), P()), out_specs=(row_spec, slot_spec, slot_spec, slot_spec), check_vma=False)
```

```python
import jax
import jax.numpy as jnp
from jax import lax
from jax.experimental import pallas as pl
from jax.experimental.pallas import tpu as pltpu
from jax.sharding import PartitionSpec as P

MESH = pl.DeviceIdType.MESH
BF16, F32 = jnp.bfloat16, jnp.float32
ANY = pl.BlockSpec(memory_space=pl.ANY)
VMEM = pl.BlockSpec(memory_space=pltpu.VMEM)
SMEM = pl.BlockSpec(memory_space=pltpu.SMEM)
HBM = pl.BlockSpec(memory_space=pltpu.HBM)
MIB = 1024 * 1024
HELD = 1
EARLY, SECOND, THIRD = 7, 4, 4
FIRST = EARLY + 1


def places():
    me = lax.axis_index('ep')
    core, chip = me % 2, me // 2
    x, y = chip % 2, chip // 2
    sib = chip * 2 + 1 - core
    chips = ((1 - y) * 2 + 1 - x, y * 2 + 1 - x, (1 - y) * 2 + x)
    return me, core, chip, sib, chips


def enter(partners):
    barrier = pltpu.get_barrier_semaphore()
    for dev in partners:
        pl.semaphore_signal(barrier, inc=1, device_id={'ep': dev}, device_id_type=MESH)
    pl.semaphore_wait(barrier, len(partners))


def remote(src, dst, send, recv, dev):
    return pltpu.make_async_remote_copy(src, dst, send, recv, device_id={'ep': dev}, device_id_type=MESH)


def pack_kernel(src, wg, wu, wd, mine_ref, chip_ref, send_ref, own_ref, sem):
    me = lax.axis_index('ep')
    slots, depth, width = wg.shape
    owner = [src[i] // slots for i in range(2)]
    mine_ref[0] = jnp.where((owner[0] == me) | (owner[1] == me), 1, 0)
    chip_ref[0] = jnp.where((owner[0] // 2 == me // 2) | (owner[1] // 2 == me // 2), 1, 0)
    half = 3 * depth // 2
    slot = jnp.where(src[0] // slots == me, src[0], src[1]) % slots

    def first(ref, k):
        return [pltpu.make_async_copy(wg.at[slot], ref.at[pl.ds(0, depth)], sem.at[k]),
                pltpu.make_async_copy(wu.at[slot, pl.ds(0, half - depth)], ref.at[pl.ds(depth, half - depth)], sem.at[k + 1])]

    def second(ref, k):
        rest = 2 * depth - half
        copies = [pltpu.make_async_copy(wu.at[slot, pl.ds(half - depth, rest)], ref.at[pl.ds(0, rest)], sem.at[k])]
        for b in range(depth // width):
            copies.append(pltpu.make_async_copy(wd.at[slot, :, pl.ds(width * b, width)],
                                                ref.at[pl.ds(rest + width * b, width)], sem.at[k + 1 + b]))
        return copies

    def run(copies):
        for copy in copies:
            copy.start()
        for copy in copies:
            copy.wait()

    @pl.when(me % 2 == 0)
    def _():
        run(second(send_ref, 2) + first(own_ref, 0))

    @pl.when(me % 2 == 1)
    def _():
        run(first(send_ref, 0) + second(own_ref, 2))


def dispatch_kernel(mine_ref, x_ref, ids_ref, gate_ref, slot_ref, own, wg, wu, wd, xall, iall, gall, near, h0, h1, h2, h3, *rest):
    me, core, chip, sib, chips = places()
    peers = [c * 2 + core for c in chips]
    bufs, (send, recv, sem) = rest[:-3], rest[-3:]
    per = len(bufs) // 3
    size = EARLY // per
    reads = [pltpu.make_async_copy(w.at[pl.ds(i * size, size)], bufs[k * per + i], sem.at[k * per + i])
             for i in range(per) for k, w in enumerate((wg, wu, wd))]
    for copy in reads:
        copy.start()
    enter(peers + [sib])

    alls = (xall, iall, gall)

    def group(k, refs, block, dev):
        return [remote(ref, to.at[block], send.at[3 * k + n], recv.at[3 * k + n], dev)
                for n, (ref, to) in enumerate(zip(refs, alls))]

    mine = (x_ref, ids_ref, gate_ref)
    first = [group(k, mine, me, dev) for k, dev in enumerate(peers + [sib])]
    for copies in first:
        for copy in copies:
            copy.start()
    slot = remote(slot_ref, near, send.at[21], recv.at[21], sib)
    slot.start()
    for ref, to in zip(mine, alls):
        to[pl.ds(me, 1)] = ref[...][None]
    slot.wait_recv()
    part = h0.shape[0]
    for k, held in enumerate((h0, h1, h2, h3)):
        rows = pl.ds(k * part, part)
        held[...] = jnp.where(mine_ref[0] > 0, own[rows, :], near[rows, :])
    second = []
    for k in (1, 2, 0):
        for copy in first[k]:
            copy.wait_recv()
        fwd = group(4 + k, [to.at[peers[k]] for to in alls], peers[k], sib)
        for copy in fwd:
            copy.start()
        second.append(fwd)
    for copy in first[3]:
        copy.wait_recv()
    for copies in first:
        for copy in copies:
            copy.wait_send()
    for copies in second:
        for copy in copies:
            copy.wait()
    slot.wait_send()
    for copy in reads:
        copy.wait()


def lands(src, dst, slot, slots):
    me = lax.axis_index('ep')
    local = (src[0] // slots == me) & (src[1] // slots == me)
    for i in range(2):
        slot = jnp.where(local & (slot == src[i] % slots), dst[i] % slots + slots, slot)
    return slot % slots


def stream(src, dst, slots0, w, w_new, bufs, sem_in, sem_out):
    def load(i):
        return [pltpu.make_async_copy(w[k].at[slots0 + i], bufs[k].at[i], sem_in.at[k, i]) for k in range(3)]

    def drain(i):
        to = lands(src, dst, slots0 + i, w[0].shape[0])
        return [pltpu.make_async_copy(bufs[k].at[i], w_new[k].at[to], sem_out.at[k, i]) for k in range(3)]

    return load, drain


def experts(i, xs, gate, bufs):
    act_g = jnp.dot(xs, bufs[0][i], preferred_element_type=F32)
    act_u = jnp.dot(xs, bufs[1][i], preferred_element_type=F32)
    z = (jax.nn.silu(act_g) * act_u).astype(BF16)
    o = jnp.dot(z, bufs[2][i], preferred_element_type=F32)
    return (o * gate).astype(BF16)


def first_kernel(src, dst, old_map, x_ref, iall, gall, *rest):
    bufs, rest = rest[:-21], rest[-21:]
    wg, wu, wd, wg_new, wu_new, wd_new, xg_out, at_ref, gr_out, c_ref, eg, eu, ed, xg, a_ref, gr_ref, pos, gsc = rest[:18]
    more_in, more_out, sem_out = rest[18:]
    me = lax.axis_index('ep')
    slots, tok, cap = wg_new.shape[0], 64, 8
    total = x_ref.shape[0]
    devs = total // tok
    rows = devs * cap
    done = FIRST * rows
    more = (eg, eu, ed)
    load, drain = stream(src, dst, EARLY, (wg, wu, wd), (wg_new, wu_new, wd_new), more, more_in, more_out)
    for i in range(FIRST - EARLY):
        for copy in load(i):
            copy.start()
    held = len(bufs) // 3
    size = EARLY // held
    drains = [pltpu.make_async_copy(bufs[k * held + i].at[0], new.at[lands(src, dst, i, slots)], sem_out.at[k, i])
              for i in range(held) for k, new in enumerate((wg_new, wu_new, wd_new))]
    for copy in drains:
        copy.start()

    ids = jnp.concatenate([iall[d].astype(F32) for d in range(devs)], axis=1)
    gates = jnp.concatenate([gall[d] for d in range(devs)], axis=1)
    hits, gs = [], []
    for j in range(slots):
        same = ids == old_map[me * slots + j].astype(F32)
        hits.append(jnp.sum(jnp.where(same, 1.0, 0.0), axis=0, keepdims=True))
        gs.append(jnp.sum(jnp.where(same, gates, 0.0), axis=0, keepdims=True))
    hit = jnp.concatenate(hits, axis=0)
    gsc[...] = jnp.concatenate(gs, axis=0)
    t_row = lax.broadcasted_iota(jnp.int32, (total, total), 0)
    t_col = lax.broadcasted_iota(jnp.int32, (total, total), 1)
    before = jnp.where((t_row < t_col) & (t_row // tok == t_col // tok), 1.0, 0.0).astype(BF16)
    rank = jnp.dot(hit.astype(BF16), before, preferred_element_type=F32)
    owner = (lax.broadcasted_iota(jnp.int32, (slots, total), 1) // tok * cap).astype(F32)
    pos[...] = jnp.where(hit > 0.5, rank + owner, -1.0)
    post = jnp.transpose(jnp.concatenate([pos[...], jnp.full((128 - slots, total), -1.0, F32)], axis=0))
    wide = lax.broadcasted_iota(jnp.int32, (total, 128), 1)
    for p in range(slots // 2):
        want = jnp.where(wide < rows, post[:, 2 * p:2 * p + 1], post[:, 2 * p + 1:2 * p + 2])
        at_ref[:, pl.ds(128 * p, 128)] = jnp.where(want == (wide % rows).astype(F32), 1.0, 0.0).astype(BF16)

    row_id = lax.broadcasted_iota(jnp.int32, (rows, total), 0).astype(F32)

    def choose(first, count, g_ref):
        @pl.loop(0, count)
        def _(j):
            chosen = row_id == pos[pl.ds(first + j, 1), :]
            a_ref[pl.ds(pl.multiple_of((first + j) * rows, rows), rows), :] = jnp.where(chosen, 1.0, 0.0).astype(BF16)
            g = jnp.sum(jnp.where(chosen, gsc[pl.ds(first + j, 1), :], 0.0), axis=1, keepdims=True)
            g_ref[pl.ds(pl.multiple_of(j * rows, rows), rows), :] = jnp.broadcast_to(g, (rows, 128))

    def gather(first, count, to_ref):
        step = max(d for d in range(16, 257, 16) if count % d == 0)

        @pl.loop(0, count // step)
        def _(q):
            r0 = pl.multiple_of(q * step, step)
            picked = jnp.dot(a_ref[pl.ds(first + r0, step), :], x_ref[...], preferred_element_type=F32)
            to_ref[pl.ds(r0, step), :] = picked.astype(BF16)

    choose(0, FIRST, gr_ref)
    gather(0, done, xg)

    for n in range(held):
        @pl.loop(0, size)
        def _(i):
            at = pl.ds(pl.multiple_of((n * size + i) * rows, rows), rows)
            c_ref[at, :] = experts(i, xg[at, :], gr_ref[at, 0:1], bufs[n::held])

    @pl.loop(0, FIRST - EARLY)
    def _(i):
        for copy in load(i):
            copy.wait()
        for copy in drain(i):
            copy.start()
        at = pl.ds(pl.multiple_of((EARLY + i) * rows, rows), rows)
        c_ref[at, :] = experts(i, xg[at, :], gr_ref[at, 0:1], more)

    choose(FIRST, slots - FIRST, gr_out)
    gather(done, (slots - FIRST) * rows, xg_out)
    for copy in drains:
        copy.wait()
    for i in range(FIRST - EARLY):
        for copy in drain(i):
            copy.wait()


def later(src, dst, first_slot, xg, gr_ref, w, w_new, c_ref, c_base, bufs, sem_in, sem_out, begin, finish):
    count = bufs[0].shape[0]
    rows = gr_ref.shape[0] // (w[0].shape[0] - FIRST)
    load, drain = stream(src, dst, first_slot, w, w_new, bufs, sem_in, sem_out)
    for i in range(count):
        for copy in load(i):
            copy.start()
    base = (first_slot - FIRST) * rows
    begin()

    @pl.loop(0, count)
    def _(i):
        for copy in load(i):
            copy.wait()
        for copy in drain(i):
            copy.start()
        r0 = pl.multiple_of(i * rows, rows)
        at = pl.ds(pl.multiple_of(base + r0, rows), rows)
        c_ref[pl.ds(pl.multiple_of(c_base + r0, rows), rows), :] = experts(i, xg[at, :], gr_ref[at, 0:1], bufs)

    finish()
    for i in range(count):
        for copy in drain(i):
            copy.wait()


def second_kernel(src, dst, xg, gr_ref, wg, wu, wd, wg_old, wu_old, wd_old, wg_new, wu_new, wd_new, c_ref,
                  bg, bu, bd, sem_in, sem_out):
    later(src, dst, FIRST, xg, gr_ref, (wg, wu, wd), (wg_new, wu_new, wd_new), c_ref, 0, (bg, bu, bd), sem_in, sem_out,
          lambda: None, lambda: None)


def third_kernel(src, dst, xg, gr_ref, at_ref, c0, c1, wg, wu, wd, wg_old, wu_old, wd_old, wg_new, wu_new, wd_new, out_ref,
                 bg, bu, bd, c_ref, sem_in, sem_out):
    cols = 256
    n0 = c0.shape[0]
    done = n0 + c1.shape[0]

    def over_columns(sums):
        @pl.loop(0, out_ref.shape[1] // cols)
        def _(n):
            at = pl.ds(pl.multiple_of(n * cols, cols), cols)
            out_ref[:, at] = sums(at)

    def begin():
        over_columns(lambda at: jnp.dot(at_ref[:, 0:n0], c0[:, at], preferred_element_type=F32)
                     + jnp.dot(at_ref[:, n0:done], c1[:, at], preferred_element_type=F32))

    def finish():
        over_columns(lambda at: out_ref[:, at] + jnp.dot(at_ref[:, done:], c_ref[:, at], preferred_element_type=F32))

    later(src, dst, FIRST + SECOND, xg, gr_ref, (wg, wu, wd), (wg_new, wu_new, wd_new), c_ref, 0, (bg, bu, bd), sem_in, sem_out,
          begin, finish)


def combine_kernel(part, x_ref, rx1, rx2, rx3, ry1, ry2, ry3, own, y_ref, got, gown, near, summed, far, relay, last,
                   send, recv):
    me, core, chip, sib, chips = places()
    dev_x, dev_y = chips[1] * 2 + core, chips[2] * 2 + core
    order = list(chips) + [chip]
    enter([dev_x, dev_y, sib])
    across = [remote(part.at[c * 2 + 1 - core], near.at[k], send.at[k], recv.at[k], sib) for k, c in enumerate(order)]
    for copy in across:
        copy.start()
    moved = [remote(r, got.at[k], send.at[10 + k], recv.at[10 + k], sib) for k, r in enumerate((rx1, rx2, rx3, ry1, ry2, ry3))]
    moved.append(remote(own, gown, send.at[16], recv.at[16], sib))
    for copy in moved:
        copy.start()
    half = x_ref.shape[1] // 2
    cols = (pl.ds(0, half), pl.ds(half, half))
    towards = (dev_x, dev_y)
    diag = [remote(summed.at[0, :, cols[h]], far.at[0, :, cols[h]], send.at[4 + h], recv.at[4 + h], towards[h]) for h in range(2)]
    next_ = [remote(summed.at[1 + h, :, cols[h]], far.at[1, :, cols[h]], send.at[6 + h], recv.at[6 + h], towards[h]) for h in range(2)]
    onward = [remote(relay.at[h], last.at[h], send.at[8 + h], recv.at[8 + h], towards[1 - h]) for h in range(2)]
    for k in range(4):
        across[k].wait_recv()
        summed[k] = part[order[k] * 2 + core] + near[k]
        if k == 1:
            for copy in diag:
                copy.start()
        elif k == 2:
            next_[0].start()
        elif k == 3:
            next_[1].start()
    acc = x_ref[...].astype(F32) + summed[3]
    for h in range(2):
        diag[h].wait_recv()
        relay[h] = summed[2 - h, :, cols[h]] + far[0, :, cols[h]]
    for h in range(2):
        onward[h].start()
    for h in range(2):
        next_[h].wait_recv()
    acc = acc + far[1]
    for h in range(2):
        onward[h].wait_recv()
        y_ref[:, cols[h]] = (acc[:, h * half:(h + 1) * half] + last[h]).astype(BF16)
    for copy in moved:
        copy.wait_recv()
    for copy in across + diag + next_ + onward + moved:
        copy.wait_send()


def patch_kernel(dst, y_ref, rx1, rx2, rx3, ry1, ry2, ry3, got, near, gown, wg_old, wu_old, wd_old,
                 wg_new, wu_new, wd_new, y_out, sem):
    put_y = pltpu.make_async_copy(y_ref, y_out, sem.at[13])
    put_y.start()
    me = lax.axis_index('ep')
    core = me % 2
    slots, depth, width = wg_new.shape
    part = rx1.shape[0]
    count = 3 * depth // part
    owner = [dst[i] // slots for i in range(2)]
    here = [owner[i] == me for i in range(2)]
    chip = [owner[i] // 2 for i in range(2)]
    local = here[0] & here[1]
    comes = (here[0] | here[1]) & jnp.logical_not(local)
    same_x, same_y = chip[0] % 2 == chip[1] % 2, chip[0] // 2 == chip[1] // 2

    def put(refs, slot):
        spans = [(0, depth, wg_new, None), (depth, 2 * depth, wu_new, None)]
        spans += [(2 * depth + width * b, 2 * depth + width * (b + 1), wd_new, b) for b in range(depth // width)]
        copies, at = [], 0
        for ref in refs:
            n = ref.shape[0]
            for lo, hi, new, b in spans:
                r0, r1 = max(at, lo), min(at + n, hi)
                if r0 < r1:
                    rows = pl.ds(r0 - lo, r1 - r0)
                    where = new.at[slot, rows] if b is None else new.at[slot, rows, pl.ds(width * b, width)]
                    copies.append(pltpu.make_async_copy(ref.at[pl.ds(r0 - at, r1 - r0)], where, sem.at[len(copies)]))
            at += n
        for copy in copies:
            copy.start()
        for copy in copies:
            copy.wait()

    def receive(case, mine, theirs):
        for c in range(2):
            @pl.when(comes & case & (core == c))
            def _(refs=mine + theirs if c == 0 else theirs + mine):
                put(refs, jnp.where(here[0], dst[0], dst[1]) % slots)

    no = jnp.logical_not
    came = (rx1, rx2, rx3, ry1, ry2, ry3)
    for case, order in ((same_y & no(same_x), (0, 1, 2, 5)), (same_x & no(same_y), (2, 5, 4, 3)),
                        (no(same_x) & no(same_y), (4, 5, 2, 1))):
        receive(case, [came[k] for k in order], [got.at[k] for k in order])
    receive(same_y & same_x, [near], [gown])

    put_y.wait()


def cost(flops, moved):
    return pl.CostEstimate(flops=flops, bytes_accessed=moved, transcendentals=0)


def solution(mesh):
    groups = mesh.shape['ep']

    def flip(bit):
        return [(d, d + bit - 2 * bit * ((d // bit) % 2)) for d in range(groups)]

    to_x, to_y = flip(2), flip(4)

    def local_step(x_loc, expert_ids, gate_val, w_gate, w_up, w_down, old_map, mig_src, mig_dst):
        tok, model = x_loc.shape
        top = expert_ids.shape[1]
        slots, depth, width = w_gate.shape
        total = groups * tok
        per = groups * 8
        rows = slots * per
        late = (slots - FIRST) * per
        half = 3 * depth // 2
        weights = (w_gate, w_up, w_down)
        shapes = tuple(jax.ShapeDtypeStruct(w.shape, BF16) for w in weights)
        dma = pltpu.SemaphoreType.DMA
        slot_bytes = 6 * depth * width

        def params(mib, **kw):
            return pltpu.CompilerParams(vmem_limit_bytes=mib * MIB, **kw)

        def bf(*shape):
            return jax.ShapeDtypeStruct(shape, BF16)

        i_own, chip_own, send, own = pl.pallas_call(
            pack_kernel,
            out_shape=(jax.ShapeDtypeStruct((1,), jnp.int32),) * 2 + (bf(half, width),) * 2,
            in_specs=[SMEM, HBM, HBM, HBM], out_specs=(SMEM, SMEM, VMEM, VMEM),
            scratch_shapes=[dma((6,))], compiler_params=params(42),
            cost_estimate=cost(2_000_000_000, 2 * slot_bytes), name='pack',
        )(mig_src, *weights)

        part = half // 4
        xall, iall, gall, near, h0, h1, h2, h3, *bufs = pl.pallas_call(
            dispatch_kernel,
            out_shape=(bf(groups, tok, model), jax.ShapeDtypeStruct((groups, top, tok), jnp.int32),
                       jax.ShapeDtypeStruct((groups, top, tok), F32), bf(half, width))
            + (bf(part, width),) * 4 + tuple(bf(HELD, *w.shape[1:]) for w in weights for _ in range(EARLY // HELD)),
            in_specs=[SMEM, VMEM, VMEM, VMEM, ANY, VMEM, HBM, HBM, HBM], out_specs=(VMEM,) * (8 + 3 * (EARLY // HELD)),
            scratch_shapes=[dma((22,)), dma((22,)), dma((3 * (EARLY // HELD),))],
            compiler_params=params(4, collective_id=0, has_side_effects=True),
            cost_estimate=cost(8_000_000_000, 2_000_000), name='dispatch',
        )(i_own, x_loc, expert_ids.T, gate_val.T, send, own, *weights)

        chip_own = chip_own[0] > 0
        held = (h0, h1, h2, h3)

        def hop(to_x_rows, to_y_rows):
            return lax.ppermute(to_x_rows, 'ep', to_x), lax.ppermute(to_y_rows, 'ep', to_y)

        def onward(k_x, k_y, from_x, from_y, ready):
            from_x, from_y, *ready = lax.optimization_barrier((from_x, from_y, *ready))
            rows_x, rows_y = jnp.where(chip_own, held[k_x], from_y), jnp.where(chip_own, held[k_y], from_x)
            rows_x, rows_y, *ready = lax.optimization_barrier((rows_x, rows_y, *ready))
            return from_x, from_y, *hop(rows_x, rows_y), ready

        rx1, ry1 = hop(held[0], held[3])

        def room(count):
            return [pltpu.VMEM((count,) + w.shape[1:], BF16) for w in weights]

        *new, xg, at, gr, c0 = pl.pallas_call(
            first_kernel,
            out_shape=shapes + (bf(late, model), bf(total, rows), jax.ShapeDtypeStruct((late, 128), F32), bf(FIRST * per, model)),
            in_specs=[SMEM] * 3 + [VMEM] * (3 + 3 * (EARLY // HELD)) + [HBM] * 3, out_specs=(HBM,) * 3 + (VMEM,) * 4,
            scratch_shapes=room(FIRST - EARLY) + [
                pltpu.VMEM((FIRST * per, model), BF16), pltpu.VMEM((rows, total), BF16), pltpu.VMEM((FIRST * per, 128), F32),
                pltpu.VMEM((slots, total), F32), pltpu.VMEM((slots, total), F32),
                dma((3, FIRST - EARLY)), dma((3, FIRST - EARLY)), dma((3, EARLY // HELD))],
            compiler_params=params(11), cost_estimate=cost(30_000_000_000, (2 * FIRST - EARLY) * slot_bytes), name='first',
        )(mig_src, mig_dst, old_map, xall.reshape(total, model), iall, gall, *bufs, *weights)

        rx1, ry1, rx2, ry2, (xg, c0) = onward(1, 2, rx1, ry1, (xg, c0))
        *new, c1 = pl.pallas_call(
            second_kernel,
            out_shape=shapes + (bf(SECOND * per, model),),
            in_specs=[SMEM] * 2 + [VMEM] * 2 + [HBM] * 6, out_specs=(HBM,) * 3 + (VMEM,),
            input_output_aliases={7: 0, 8: 1, 9: 2},
            scratch_shapes=room(SECOND) + [dma((3, SECOND))] * 2,
            compiler_params=params(40), cost_estimate=cost(30_000_000_000, 2 * SECOND * slot_bytes), name='second',
        )(mig_src, mig_dst, xg, gr, *weights, *new)

        rx2, ry2, rx3, ry3, (xg, c1) = onward(2, 1, rx2, ry2, (xg, c1))
        *new, psum = pl.pallas_call(
            third_kernel,
            out_shape=shapes + (jax.ShapeDtypeStruct((total, model), F32),),
            in_specs=[SMEM] * 2 + [VMEM] * 5 + [HBM] * 6, out_specs=(HBM,) * 3 + (VMEM,),
            input_output_aliases={10: 0, 11: 1, 12: 2},
            scratch_shapes=room(THIRD) + [pltpu.VMEM((THIRD * per, model), BF16)] + [dma((3, THIRD))] * 2,
            compiler_params=params(40), cost_estimate=cost(30_000_000_000, 2 * THIRD * slot_bytes), name='third',
        )(mig_src, mig_dst, xg, gr, at, c0, c1, *weights, *new)

        came = (rx1, rx2, rx3, ry1, ry2, ry3)
        y_out, got, gown = pl.pallas_call(
            combine_kernel,
            out_shape=(bf(tok, model), bf(6, part, width), bf(half, width)),
            in_specs=[VMEM, VMEM] + [ANY] * 7, out_specs=(VMEM, ANY, ANY),
            scratch_shapes=[pltpu.VMEM((4, tok, model), F32), pltpu.VMEM((4, tok, model), F32),
                            pltpu.VMEM((2, tok, model), F32), pltpu.VMEM((2, tok, model // 2), F32),
                            pltpu.VMEM((2, tok, model // 2), F32), dma((17,)), dma((17,))],
            compiler_params=params(24, collective_id=1, has_side_effects=True),
            cost_estimate=cost(16_000_000_000, 4_000_000), name='combine',
        )(psum.reshape(groups, tok, model), x_loc, *came, own)

        *new, y_out = pl.pallas_call(
            patch_kernel,
            out_shape=shapes + (bf(tok, model),),
            in_specs=[SMEM] + [VMEM] * 10 + [HBM] * 3, out_specs=(HBM,) * 4,
            input_output_aliases={11: 0, 12: 1, 13: 2},
            scratch_shapes=[dma((14,))],
            compiler_params=params(40), cost_estimate=cost(3_000_000_000, 2 * slot_bytes), name='patch',
        )(mig_dst, y_out, *came, got, near, gown, *new)
        return (y_out, *new)

    row_spec = P(('dp', 'ep'), None)
    slot_spec = P('ep', None, None)
    return jax.shard_map(local_step, mesh=mesh, in_specs=(row_spec, row_spec, row_spec, slot_spec, slot_spec, slot_spec, P(), P(), P()), out_specs=(row_spec, slot_spec, slot_spec, slot_spec), check_vma=False)
```

```python
import jax
import jax.numpy as jnp
from jax import lax
from jax.experimental import pallas as pl
from jax.experimental.pallas import tpu as pltpu
from jax.sharding import PartitionSpec as P

MESH = pl.DeviceIdType.MESH
BF16, F32 = jnp.bfloat16, jnp.float32
ANY = pl.BlockSpec(memory_space=pl.ANY)
VMEM = pl.BlockSpec(memory_space=pltpu.VMEM)
SMEM = pl.BlockSpec(memory_space=pltpu.SMEM)
HBM = pl.BlockSpec(memory_space=pltpu.HBM)
MIB = 1024 * 1024
HELD = 1
EARLY, SECOND, THIRD = 7, 4, 4
FIRST = EARLY + 1


def places():
    me = lax.axis_index('ep')
    core, chip = me % 2, me // 2
    x, y = chip % 2, chip // 2
    sib = chip * 2 + 1 - core
    chips = ((1 - y) * 2 + 1 - x, y * 2 + 1 - x, (1 - y) * 2 + x)
    return me, core, chip, sib, chips


def enter(partners):
    barrier = pltpu.get_barrier_semaphore()
    for dev in partners:
        pl.semaphore_signal(barrier, inc=1, device_id={'ep': dev}, device_id_type=MESH)
    pl.semaphore_wait(barrier, len(partners))


def remote(src, dst, send, recv, dev):
    return pltpu.make_async_remote_copy(src, dst, send, recv, device_id={'ep': dev}, device_id_type=MESH)


def pack_kernel(src, wg, wu, wd, mine_ref, chip_ref, send_ref, own_ref, sem):
    me = lax.axis_index('ep')
    slots, depth, width = wg.shape
    owner = [src[i] // slots for i in range(2)]
    mine_ref[0] = jnp.where((owner[0] == me) | (owner[1] == me), 1, 0)
    chip_ref[0] = jnp.where((owner[0] // 2 == me // 2) | (owner[1] // 2 == me // 2), 1, 0)
    half = 3 * depth // 2
    slot = jnp.where(src[0] // slots == me, src[0], src[1]) % slots

    def first(ref, k):
        return [pltpu.make_async_copy(wg.at[slot], ref.at[pl.ds(0, depth)], sem.at[k]),
                pltpu.make_async_copy(wu.at[slot, pl.ds(0, half - depth)], ref.at[pl.ds(depth, half - depth)], sem.at[k + 1])]

    def second(ref, k):
        rest = 2 * depth - half
        copies = [pltpu.make_async_copy(wu.at[slot, pl.ds(half - depth, rest)], ref.at[pl.ds(0, rest)], sem.at[k])]
        for b in range(depth // width):
            copies.append(pltpu.make_async_copy(wd.at[slot, :, pl.ds(width * b, width)],
                                                ref.at[pl.ds(rest + width * b, width)], sem.at[k + 1 + b]))
        return copies

    def run(copies):
        for copy in copies:
            copy.start()
        for copy in copies:
            copy.wait()

    @pl.when(me % 2 == 0)
    def _():
        run(second(send_ref, 2) + first(own_ref, 0))

    @pl.when(me % 2 == 1)
    def _():
        run(first(send_ref, 0) + second(own_ref, 2))


def dispatch_kernel(mine_ref, x_ref, ids_ref, gate_ref, slot_ref, own, wg, wu, wd, xall, iall, gall, near, h0, h1, h2, h3, *rest):
    me, core, chip, sib, chips = places()
    peers = [c * 2 + core for c in chips]
    bufs, (send, recv, sem) = rest[:-3], rest[-3:]
    per = len(bufs) // 3
    size = EARLY // per
    reads = [pltpu.make_async_copy(w.at[pl.ds(i * size, size)], bufs[k * per + i], sem.at[k * per + i])
             for i in range(per) for k, w in enumerate((wg, wu, wd))]
    for copy in reads:
        copy.start()
    enter(peers + [sib])

    (dev_d, dev_x, dev_y), half = peers, x_ref.shape[0] // 2
    low, high = pl.ds(0, half), pl.ds(half, half)

    def rows(k, block, part, dev, ref=None):
        to = xall.at[block, part]
        return remote(to if ref is None else ref.at[part], to, send.at[k], recv.at[k], dev)

    def table(k, block, dev, refs):
        return [remote(ref, to.at[block], send.at[k + n], recv.at[k + n], dev) for n, (ref, to) in enumerate(zip(refs, (iall, gall)))]

    own_rows = {key: rows(k, me, part, dev, x_ref) for k, (key, part, dev) in enumerate((
        ('xh', high, dev_x), ('yl', low, dev_y), ('xl', low, dev_x), ('yh', high, dev_y), ('sl', low, sib), ('sh', high, sib)))}
    own_tables = [table(6 + 2 * k, me, dev, (ids_ref, gate_ref)) for k, dev in enumerate(peers + [sib])]
    slot = remote(slot_ref, near, send.at[14], recv.at[14], sib)
    for key in ('xh', 'yl'):
        own_rows[key].start()
    for copies in own_tables:
        for copy in copies:
            copy.start()
    for key in ('xl', 'yh', 'sl', 'sh'):
        own_rows[key].start()
    slot.start()
    mine, alls = (x_ref, ids_ref, gate_ref), (xall, iall, gall)
    for ref, to in zip(mine, alls):
        to[pl.ds(me, 1)] = ref[...][None]
    sent = []

    def forward(*copies):
        for copy in copies:
            copy.start()
            sent.append(copy)

    own_rows['xh'].wait_recv()
    forward(rows(15, dev_x, high, dev_y), rows(17, dev_x, high, sib))
    own_rows['yl'].wait_recv()
    forward(rows(16, dev_y, low, dev_x), rows(18, dev_y, low, sib))
    slot.wait_recv()
    part = h0.shape[0]
    for k, held in enumerate((h0, h1, h2, h3)):
        span = pl.ds(k * part, part)
        held[...] = jnp.where(mine_ref[0] > 0, own[span, :], near[span, :])
    for k, dev in enumerate(peers):
        for copy in own_tables[k]:
            copy.wait_recv()
        forward(*table(23 + 2 * k, dev, sib, (iall.at[dev], gall.at[dev])))
    own_rows['xl'].wait_recv()
    forward(rows(19, dev_x, low, sib))
    own_rows['yh'].wait_recv()
    forward(rows(20, dev_y, high, sib))
    sent[0].wait_recv()
    forward(rows(21, dev_d, high, sib))
    sent[2].wait_recv()
    forward(rows(22, dev_d, low, sib))
    for copy in own_tables[3]:
        copy.wait_recv()
    for key in ('sl', 'sh'):
        own_rows[key].wait_recv()
    for k, copy in enumerate(sent):
        if k not in (0, 2):
            copy.wait_recv()
        copy.wait_send()
    for copy in list(own_rows.values()) + [copy for copies in own_tables for copy in copies]:
        copy.wait_send()
    slot.wait_send()
    for copy in reads:
        copy.wait()


def lands(src, dst, slot, slots):
    me = lax.axis_index('ep')
    local = (src[0] // slots == me) & (src[1] // slots == me)
    for i in range(2):
        slot = jnp.where(local & (slot == src[i] % slots), dst[i] % slots + slots, slot)
    return slot % slots


def stream(src, dst, slots0, w, w_new, bufs, sem_in, sem_out):
    def load(i):
        return [pltpu.make_async_copy(w[k].at[slots0 + i], bufs[k].at[i], sem_in.at[k, i]) for k in range(3)]

    def drain(i):
        to = lands(src, dst, slots0 + i, w[0].shape[0])
        return [pltpu.make_async_copy(bufs[k].at[i], w_new[k].at[to], sem_out.at[k, i]) for k in range(3)]

    return load, drain


def experts(i, xs, gate, bufs):
    act_g = jnp.dot(xs, bufs[0][i], preferred_element_type=F32)
    act_u = jnp.dot(xs, bufs[1][i], preferred_element_type=F32)
    z = (jax.nn.silu(act_g) * act_u).astype(BF16)
    o = jnp.dot(z, bufs[2][i], preferred_element_type=F32)
    return (o * gate).astype(BF16)


def first_kernel(src, dst, old_map, x_ref, iall, gall, *rest):
    bufs, rest = rest[:-21], rest[-21:]
    wg, wu, wd, wg_new, wu_new, wd_new, xg_out, at_ref, gr_out, c_ref, eg, eu, ed, xg, a_ref, gr_ref, pos, gsc = rest[:18]
    more_in, more_out, sem_out = rest[18:]
    me = lax.axis_index('ep')
    slots, tok, cap = wg_new.shape[0], 64, 8
    total = x_ref.shape[0]
    devs = total // tok
    rows = devs * cap
    done = FIRST * rows
    more = (eg, eu, ed)
    load, drain = stream(src, dst, EARLY, (wg, wu, wd), (wg_new, wu_new, wd_new), more, more_in, more_out)
    for i in range(FIRST - EARLY):
        for copy in load(i):
            copy.start()
    held = len(bufs) // 3
    size = EARLY // held
    drains = [pltpu.make_async_copy(bufs[k * held + i].at[0], new.at[lands(src, dst, i, slots)], sem_out.at[k, i])
              for i in range(held) for k, new in enumerate((wg_new, wu_new, wd_new))]
    for copy in drains:
        copy.start()

    ids = jnp.concatenate([iall[d].astype(F32) for d in range(devs)], axis=1)
    gates = jnp.concatenate([gall[d] for d in range(devs)], axis=1)
    hits, gs = [], []
    for j in range(slots):
        same = ids == old_map[me * slots + j].astype(F32)
        hits.append(jnp.sum(jnp.where(same, 1.0, 0.0), axis=0, keepdims=True))
        gs.append(jnp.sum(jnp.where(same, gates, 0.0), axis=0, keepdims=True))
    hit = jnp.concatenate(hits, axis=0)
    gsc[...] = jnp.concatenate(gs, axis=0)
    t_row = lax.broadcasted_iota(jnp.int32, (total, total), 0)
    t_col = lax.broadcasted_iota(jnp.int32, (total, total), 1)
    before = jnp.where((t_row < t_col) & (t_row // tok == t_col // tok), 1.0, 0.0).astype(BF16)
    rank = jnp.dot(hit.astype(BF16), before, preferred_element_type=F32)
    owner = (lax.broadcasted_iota(jnp.int32, (slots, total), 1) // tok * cap).astype(F32)
    pos[...] = jnp.where(hit > 0.5, rank + owner, -1.0)
    post = jnp.transpose(jnp.concatenate([pos[...], jnp.full((128 - slots, total), -1.0, F32)], axis=0))
    wide = lax.broadcasted_iota(jnp.int32, (total, 128), 1)
    for p in range(slots // 2):
        want = jnp.where(wide < rows, post[:, 2 * p:2 * p + 1], post[:, 2 * p + 1:2 * p + 2])
        at_ref[:, pl.ds(128 * p, 128)] = jnp.where(want == (wide % rows).astype(F32), 1.0, 0.0).astype(BF16)

    row_id = lax.broadcasted_iota(jnp.int32, (rows, total), 0).astype(F32)

    def choose(first, count, g_ref):
        @pl.loop(0, count)
        def _(j):
            chosen = row_id == pos[pl.ds(first + j, 1), :]
            a_ref[pl.ds(pl.multiple_of((first + j) * rows, rows), rows), :] = jnp.where(chosen, 1.0, 0.0).astype(BF16)
            g = jnp.sum(jnp.where(chosen, gsc[pl.ds(first + j, 1), :], 0.0), axis=1, keepdims=True)
            g_ref[pl.ds(pl.multiple_of(j * rows, rows), rows), :] = jnp.broadcast_to(g, (rows, 128))

    def gather(first, count, to_ref):
        step = max(d for d in range(16, 257, 16) if count % d == 0)

        @pl.loop(0, count // step)
        def _(q):
            r0 = pl.multiple_of(q * step, step)
            picked = jnp.dot(a_ref[pl.ds(first + r0, step), :], x_ref[...], preferred_element_type=F32)
            to_ref[pl.ds(r0, step), :] = picked.astype(BF16)

    choose(0, FIRST, gr_ref)
    gather(0, done, xg)

    for n in range(held):
        @pl.loop(0, size)
        def _(i):
            at = pl.ds(pl.multiple_of((n * size + i) * rows, rows), rows)
            c_ref[at, :] = experts(i, xg[at, :], gr_ref[at, 0:1], bufs[n::held])

    @pl.loop(0, FIRST - EARLY)
    def _(i):
        for copy in load(i):
            copy.wait()
        for copy in drain(i):
            copy.start()
        at = pl.ds(pl.multiple_of((EARLY + i) * rows, rows), rows)
        c_ref[at, :] = experts(i, xg[at, :], gr_ref[at, 0:1], more)

    choose(FIRST, slots - FIRST, gr_out)
    gather(done, (slots - FIRST) * rows, xg_out)
    for copy in drains:
        copy.wait()
    for i in range(FIRST - EARLY):
        for copy in drain(i):
            copy.wait()


def later(src, dst, first_slot, xg, gr_ref, w, w_new, c_ref, c_base, bufs, sem_in, sem_out, begin, finish):
    count = bufs[0].shape[0]
    rows = gr_ref.shape[0] // (w[0].shape[0] - FIRST)
    load, drain = stream(src, dst, first_slot, w, w_new, bufs, sem_in, sem_out)
    for i in range(count):
        for copy in load(i):
            copy.start()
    base = (first_slot - FIRST) * rows
    begin()

    @pl.loop(0, count)
    def _(i):
        for copy in load(i):
            copy.wait()
        for copy in drain(i):
            copy.start()
        r0 = pl.multiple_of(i * rows, rows)
        at = pl.ds(pl.multiple_of(base + r0, rows), rows)
        c_ref[pl.ds(pl.multiple_of(c_base + r0, rows), rows), :] = experts(i, xg[at, :], gr_ref[at, 0:1], bufs)

    finish()
    for i in range(count):
        for copy in drain(i):
            copy.wait()


def second_kernel(src, dst, xg, gr_ref, wg, wu, wd, wg_old, wu_old, wd_old, wg_new, wu_new, wd_new, c_ref,
                  bg, bu, bd, sem_in, sem_out):
    later(src, dst, FIRST, xg, gr_ref, (wg, wu, wd), (wg_new, wu_new, wd_new), c_ref, 0, (bg, bu, bd), sem_in, sem_out,
          lambda: None, lambda: None)


def third_kernel(src, dst, xg, gr_ref, at_ref, c0, c1, wg, wu, wd, wg_old, wu_old, wd_old, wg_new, wu_new, wd_new, out_ref,
                 bg, bu, bd, c_ref, sem_in, sem_out):
    cols = 256
    n0 = c0.shape[0]
    done = n0 + c1.shape[0]

    def over_columns(sums):
        @pl.loop(0, out_ref.shape[1] // cols)
        def _(n):
            at = pl.ds(pl.multiple_of(n * cols, cols), cols)
            out_ref[:, at] = sums(at)

    def begin():
        over_columns(lambda at: jnp.dot(at_ref[:, 0:n0], c0[:, at], preferred_element_type=F32)
                     + jnp.dot(at_ref[:, n0:done], c1[:, at], preferred_element_type=F32))

    def finish():
        over_columns(lambda at: out_ref[:, at] + jnp.dot(at_ref[:, done:], c_ref[:, at], preferred_element_type=F32))

    later(src, dst, FIRST + SECOND, xg, gr_ref, (wg, wu, wd), (wg_new, wu_new, wd_new), c_ref, 0, (bg, bu, bd), sem_in, sem_out,
          begin, finish)


def combine_kernel(part, x_ref, rx1, rx2, rx3, ry1, ry2, ry3, own, y_ref, got, gown, near, summed, far, relay, last,
                   send, recv):
    me, core, chip, sib, chips = places()
    dev_x, dev_y = chips[1] * 2 + core, chips[2] * 2 + core
    order = list(chips) + [chip]
    enter([dev_x, dev_y, sib])
    across = [remote(part.at[c * 2 + 1 - core], near.at[k], send.at[k], recv.at[k], sib) for k, c in enumerate(order)]
    for copy in across:
        copy.start()
    moved = [remote(r, got.at[k], send.at[10 + k], recv.at[10 + k], sib) for k, r in enumerate((rx1, rx2, rx3, ry1, ry2, ry3))]
    moved.append(remote(own, gown, send.at[16], recv.at[16], sib))
    for copy in moved:
        copy.start()
    half = x_ref.shape[1] // 2
    cols = (pl.ds(0, half), pl.ds(half, half))
    towards = (dev_x, dev_y)
    diag = [remote(summed.at[0, :, cols[h]], far.at[0, :, cols[h]], send.at[4 + h], recv.at[4 + h], towards[h]) for h in range(2)]
    next_ = [remote(summed.at[1 + h, :, cols[h]], far.at[1, :, cols[h]], send.at[6 + h], recv.at[6 + h], towards[h]) for h in range(2)]
    onward = [remote(relay.at[h], last.at[h], send.at[8 + h], recv.at[8 + h], towards[1 - h]) for h in range(2)]
    for k in range(4):
        across[k].wait_recv()
        summed[k] = part[order[k] * 2 + core] + near[k]
        if k == 1:
            for copy in diag:
                copy.start()
        elif k == 2:
            next_[0].start()
        elif k == 3:
            next_[1].start()
    acc = x_ref[...].astype(F32) + summed[3]
    for h in range(2):
        diag[h].wait_recv()
        relay[h] = summed[2 - h, :, cols[h]] + far[0, :, cols[h]]
    for h in range(2):
        onward[h].start()
    for h in range(2):
        next_[h].wait_recv()
    acc = acc + far[1]
    for h in range(2):
        onward[h].wait_recv()
        y_ref[:, cols[h]] = (acc[:, h * half:(h + 1) * half] + last[h]).astype(BF16)
    for copy in moved:
        copy.wait_recv()
    for copy in across + diag + next_ + onward + moved:
        copy.wait_send()


def patch_kernel(dst, y_ref, rx1, rx2, rx3, ry1, ry2, ry3, got, near, gown, wg_old, wu_old, wd_old,
                 wg_new, wu_new, wd_new, y_out, sem):
    put_y = pltpu.make_async_copy(y_ref, y_out, sem.at[13])
    put_y.start()
    me = lax.axis_index('ep')
    core = me % 2
    slots, depth, width = wg_new.shape
    part = rx1.shape[0]
    count = 3 * depth // part
    owner = [dst[i] // slots for i in range(2)]
    here = [owner[i] == me for i in range(2)]
    chip = [owner[i] // 2 for i in range(2)]
    local = here[0] & here[1]
    comes = (here[0] | here[1]) & jnp.logical_not(local)
    same_x, same_y = chip[0] % 2 == chip[1] % 2, chip[0] // 2 == chip[1] // 2

    def put(refs, slot):
        spans = [(0, depth, wg_new, None), (depth, 2 * depth, wu_new, None)]
        spans += [(2 * depth + width * b, 2 * depth + width * (b + 1), wd_new, b) for b in range(depth // width)]
        copies, at = [], 0
        for ref in refs:
            n = ref.shape[0]
            for lo, hi, new, b in spans:
                r0, r1 = max(at, lo), min(at + n, hi)
                if r0 < r1:
                    rows = pl.ds(r0 - lo, r1 - r0)
                    where = new.at[slot, rows] if b is None else new.at[slot, rows, pl.ds(width * b, width)]
                    copies.append(pltpu.make_async_copy(ref.at[pl.ds(r0 - at, r1 - r0)], where, sem.at[len(copies)]))
            at += n
        for copy in copies:
            copy.start()
        for copy in copies:
            copy.wait()

    def receive(case, mine, theirs):
        for c in range(2):
            @pl.when(comes & case & (core == c))
            def _(refs=mine + theirs if c == 0 else theirs + mine):
                put(refs, jnp.where(here[0], dst[0], dst[1]) % slots)

    no = jnp.logical_not
    came = (rx1, rx2, rx3, ry1, ry2, ry3)
    for case, order in ((same_y & no(same_x), (0, 1, 2, 5)), (same_x & no(same_y), (2, 5, 4, 3)),
                        (no(same_x) & no(same_y), (4, 5, 2, 1))):
        receive(case, [came[k] for k in order], [got.at[k] for k in order])
    receive(same_y & same_x, [near], [gown])

    put_y.wait()


def cost(flops, moved):
    return pl.CostEstimate(flops=flops, bytes_accessed=moved, transcendentals=0)


def solution(mesh):
    groups = mesh.shape['ep']

    def flip(bit):
        return [(d, d + bit - 2 * bit * ((d // bit) % 2)) for d in range(groups)]

    to_x, to_y = flip(2), flip(4)

    def local_step(x_loc, expert_ids, gate_val, w_gate, w_up, w_down, old_map, mig_src, mig_dst):
        tok, model = x_loc.shape
        top = expert_ids.shape[1]
        slots, depth, width = w_gate.shape
        total = groups * tok
        per = groups * 8
        rows = slots * per
        late = (slots - FIRST) * per
        half = 3 * depth // 2
        weights = (w_gate, w_up, w_down)
        shapes = tuple(jax.ShapeDtypeStruct(w.shape, BF16) for w in weights)
        dma = pltpu.SemaphoreType.DMA
        slot_bytes = 6 * depth * width

        def params(mib, **kw):
            return pltpu.CompilerParams(vmem_limit_bytes=mib * MIB, **kw)

        def bf(*shape):
            return jax.ShapeDtypeStruct(shape, BF16)

        i_own, chip_own, send, own = pl.pallas_call(
            pack_kernel,
            out_shape=(jax.ShapeDtypeStruct((1,), jnp.int32),) * 2 + (bf(half, width),) * 2,
            in_specs=[SMEM, HBM, HBM, HBM], out_specs=(SMEM, SMEM, VMEM, VMEM),
            scratch_shapes=[dma((6,))], compiler_params=params(42),
            cost_estimate=cost(2_000_000_000, 2 * slot_bytes), name='pack',
        )(mig_src, *weights)

        part = half // 4
        xall, iall, gall, near, h0, h1, h2, h3, *bufs = pl.pallas_call(
            dispatch_kernel,
            out_shape=(bf(groups, tok, model), jax.ShapeDtypeStruct((groups, top, tok), jnp.int32),
                       jax.ShapeDtypeStruct((groups, top, tok), F32), bf(half, width))
            + (bf(part, width),) * 4 + tuple(bf(HELD, *w.shape[1:]) for w in weights for _ in range(EARLY // HELD)),
            in_specs=[SMEM, VMEM, VMEM, VMEM, ANY, VMEM, HBM, HBM, HBM], out_specs=(VMEM,) * (8 + 3 * (EARLY // HELD)),
            scratch_shapes=[dma((29,)), dma((29,)), dma((3 * (EARLY // HELD),))],
            compiler_params=params(4, collective_id=0, has_side_effects=True),
            cost_estimate=cost(8_000_000_000, 2_000_000), name='dispatch',
        )(i_own, x_loc, expert_ids.T, gate_val.T, send, own, *weights)

        chip_own = chip_own[0] > 0
        held = (h0, h1, h2, h3)

        def hop(to_x_rows, to_y_rows):
            return lax.ppermute(to_x_rows, 'ep', to_x), lax.ppermute(to_y_rows, 'ep', to_y)

        def onward(k_x, k_y, from_x, from_y, ready):
            from_x, from_y, *ready = lax.optimization_barrier((from_x, from_y, *ready))
            rows_x, rows_y = jnp.where(chip_own, held[k_x], from_y), jnp.where(chip_own, held[k_y], from_x)
            rows_x, rows_y, *ready = lax.optimization_barrier((rows_x, rows_y, *ready))
            return from_x, from_y, *hop(rows_x, rows_y), ready

        rx1, ry1 = hop(held[0], held[3])

        def room(count):
            return [pltpu.VMEM((count,) + w.shape[1:], BF16) for w in weights]

        *new, xg, at, gr, c0 = pl.pallas_call(
            first_kernel,
            out_shape=shapes + (bf(late, model), bf(total, rows), jax.ShapeDtypeStruct((late, 128), F32), bf(FIRST * per, model)),
            in_specs=[SMEM] * 3 + [VMEM] * (3 + 3 * (EARLY // HELD)) + [HBM] * 3, out_specs=(HBM,) * 3 + (VMEM,) * 4,
            scratch_shapes=room(FIRST - EARLY) + [
                pltpu.VMEM((FIRST * per, model), BF16), pltpu.VMEM((rows, total), BF16), pltpu.VMEM((FIRST * per, 128), F32),
                pltpu.VMEM((slots, total), F32), pltpu.VMEM((slots, total), F32),
                dma((3, FIRST - EARLY)), dma((3, FIRST - EARLY)), dma((3, EARLY // HELD))],
            compiler_params=params(11), cost_estimate=cost(30_000_000_000, (2 * FIRST - EARLY) * slot_bytes), name='first',
        )(mig_src, mig_dst, old_map, xall.reshape(total, model), iall, gall, *bufs, *weights)

        rx1, ry1, rx2, ry2, (xg, c0) = onward(1, 2, rx1, ry1, (xg, c0))
        *new, c1 = pl.pallas_call(
            second_kernel,
            out_shape=shapes + (bf(SECOND * per, model),),
            in_specs=[SMEM] * 2 + [VMEM] * 2 + [HBM] * 6, out_specs=(HBM,) * 3 + (VMEM,),
            input_output_aliases={7: 0, 8: 1, 9: 2},
            scratch_shapes=room(SECOND) + [dma((3, SECOND))] * 2,
            compiler_params=params(40), cost_estimate=cost(30_000_000_000, 2 * SECOND * slot_bytes), name='second',
        )(mig_src, mig_dst, xg, gr, *weights, *new)

        rx2, ry2, rx3, ry3, (xg, c1) = onward(2, 1, rx2, ry2, (xg, c1))
        *new, psum = pl.pallas_call(
            third_kernel,
            out_shape=shapes + (jax.ShapeDtypeStruct((total, model), F32),),
            in_specs=[SMEM] * 2 + [VMEM] * 5 + [HBM] * 6, out_specs=(HBM,) * 3 + (VMEM,),
            input_output_aliases={10: 0, 11: 1, 12: 2},
            scratch_shapes=room(THIRD) + [pltpu.VMEM((THIRD * per, model), BF16)] + [dma((3, THIRD))] * 2,
            compiler_params=params(40), cost_estimate=cost(30_000_000_000, 2 * THIRD * slot_bytes), name='third',
        )(mig_src, mig_dst, xg, gr, at, c0, c1, *weights, *new)

        came = (rx1, rx2, rx3, ry1, ry2, ry3)
        y_out, got, gown = pl.pallas_call(
            combine_kernel,
            out_shape=(bf(tok, model), bf(6, part, width), bf(half, width)),
            in_specs=[VMEM, VMEM] + [ANY] * 7, out_specs=(VMEM, ANY, ANY),
            scratch_shapes=[pltpu.VMEM((4, tok, model), F32), pltpu.VMEM((4, tok, model), F32),
                            pltpu.VMEM((2, tok, model), F32), pltpu.VMEM((2, tok, model // 2), F32),
                            pltpu.VMEM((2, tok, model // 2), F32), dma((17,)), dma((17,))],
            compiler_params=params(24, collective_id=1, has_side_effects=True),
            cost_estimate=cost(16_000_000_000, 4_000_000), name='combine',
        )(psum.reshape(groups, tok, model), x_loc, *came, own)

        *new, y_out = pl.pallas_call(
            patch_kernel,
            out_shape=shapes + (bf(tok, model),),
            in_specs=[SMEM] + [VMEM] * 10 + [HBM] * 3, out_specs=(HBM,) * 4,
            input_output_aliases={11: 0, 12: 1, 13: 2},
            scratch_shapes=[dma((14,))],
            compiler_params=params(40), cost_estimate=cost(3_000_000_000, 2 * slot_bytes), name='patch',
        )(mig_dst, y_out, *came, got, near, gown, *new)
        return (y_out, *new)

    row_spec = P(('dp', 'ep'), None)
    slot_spec = P('ep', None, None)
    return jax.shard_map(local_step, mesh=mesh, in_specs=(row_spec, row_spec, row_spec, slot_spec, slot_spec, slot_spec, P(), P(), P()), out_specs=(row_spec, slot_spec, slot_spec, slot_spec), check_vma=False)
```

```python
import jax
import jax.numpy as jnp
from jax import lax
from jax.experimental import pallas as pl
from jax.experimental.pallas import tpu as pltpu
from jax.sharding import PartitionSpec as P

MESH = pl.DeviceIdType.MESH
BF16, F32 = jnp.bfloat16, jnp.float32
ANY = pl.BlockSpec(memory_space=pl.ANY)
VMEM = pl.BlockSpec(memory_space=pltpu.VMEM)
SMEM = pl.BlockSpec(memory_space=pltpu.SMEM)
HBM = pl.BlockSpec(memory_space=pltpu.HBM)
MIB = 1024 * 1024
HELD = 1
EARLY, SECOND, THIRD = 7, 4, 4
FIRST = EARLY + 1


def places():
    me = lax.axis_index('ep')
    core, chip = me % 2, me // 2
    x, y = chip % 2, chip // 2
    sib = chip * 2 + 1 - core
    chips = ((1 - y) * 2 + 1 - x, y * 2 + 1 - x, (1 - y) * 2 + x)
    return me, core, chip, sib, chips


def enter(partners):
    barrier = pltpu.get_barrier_semaphore()
    for dev in partners:
        pl.semaphore_signal(barrier, inc=1, device_id={'ep': dev}, device_id_type=MESH)
    pl.semaphore_wait(barrier, len(partners))


def remote(src, dst, send, recv, dev):
    return pltpu.make_async_remote_copy(src, dst, send, recv, device_id={'ep': dev}, device_id_type=MESH)


def pack_kernel(src, wg, wu, wd, mine_ref, chip_ref, send_ref, own_ref, sem):
    me = lax.axis_index('ep')
    slots, depth, width = wg.shape
    owner = [src[i] // slots for i in range(2)]
    mine_ref[0] = jnp.where((owner[0] == me) | (owner[1] == me), 1, 0)
    chip_ref[0] = jnp.where((owner[0] // 2 == me // 2) | (owner[1] // 2 == me // 2), 1, 0)
    half = 3 * depth // 2
    slot = jnp.where(src[0] // slots == me, src[0], src[1]) % slots

    def first(ref, k):
        return [pltpu.make_async_copy(wg.at[slot], ref.at[pl.ds(0, depth)], sem.at[k]),
                pltpu.make_async_copy(wu.at[slot, pl.ds(0, half - depth)], ref.at[pl.ds(depth, half - depth)], sem.at[k + 1])]

    def second(ref, k):
        rest = 2 * depth - half
        copies = [pltpu.make_async_copy(wu.at[slot, pl.ds(half - depth, rest)], ref.at[pl.ds(0, rest)], sem.at[k])]
        for b in range(depth // width):
            copies.append(pltpu.make_async_copy(wd.at[slot, :, pl.ds(width * b, width)],
                                                ref.at[pl.ds(rest + width * b, width)], sem.at[k + 1 + b]))
        return copies

    def run(copies):
        for copy in copies:
            copy.start()
        for copy in copies:
            copy.wait()

    @pl.when(me % 2 == 0)
    def _():
        run(second(send_ref, 2) + first(own_ref, 0))

    @pl.when(me % 2 == 1)
    def _():
        run(first(send_ref, 0) + second(own_ref, 2))


def dispatch_kernel(mine_ref, x_ref, ids_ref, gate_ref, slot_ref, own, wg, wu, wd, xall, iall, gall, near, h0, h1, h2, h3, *rest):
    me, core, chip, sib, chips = places()
    peers = [c * 2 + core for c in chips]
    bufs, (send, recv, sem) = rest[:-3], rest[-3:]
    per = len(bufs) // 3
    size = EARLY // per
    reads = [pltpu.make_async_copy(w.at[pl.ds(i * size, size)], bufs[k * per + i], sem.at[k * per + i])
             for i in range(per) for k, w in enumerate((wg, wu, wd))]
    for copy in reads:
        copy.start()
    enter(peers + [sib])

    (dev_d, dev_x, dev_y), half = peers, x_ref.shape[0] // 2
    low, high = pl.ds(0, half), pl.ds(half, half)

    def rows(k, block, part, dev, ref=None):
        to = xall.at[block, part]
        return remote(to if ref is None else ref.at[part], to, send.at[k], recv.at[k], dev)

    def table(k, block, dev, refs):
        return [remote(ref, to.at[block], send.at[k + n], recv.at[k + n], dev) for n, (ref, to) in enumerate(zip(refs, (iall, gall)))]

    own_rows = {key: rows(k, me, part, dev, x_ref) for k, (key, part, dev) in enumerate((
        ('xh', high, dev_x), ('yl', low, dev_y), ('xl', low, dev_x), ('yh', high, dev_y), ('sl', low, sib), ('sh', high, sib)))}
    own_tables = [table(6 + 2 * k, me, dev, (ids_ref, gate_ref)) for k, dev in enumerate(peers + [sib])]
    slot = remote(slot_ref, near, send.at[14], recv.at[14], sib)
    for key in ('xh', 'yl'):
        own_rows[key].start()
    for copies in own_tables:
        for copy in copies:
            copy.start()
    for key in ('xl', 'yh', 'sl', 'sh'):
        own_rows[key].start()
    slot.start()
    mine, alls = (x_ref, ids_ref, gate_ref), (xall, iall, gall)
    for ref, to in zip(mine, alls):
        to[pl.ds(me, 1)] = ref[...][None]
    sent = []

    def forward(*copies):
        for copy in copies:
            copy.start()
            sent.append(copy)

    own_rows['xh'].wait_recv()
    forward(rows(15, dev_x, high, dev_y), rows(17, dev_x, high, sib))
    own_rows['yl'].wait_recv()
    forward(rows(16, dev_y, low, dev_x), rows(18, dev_y, low, sib))
    slot.wait_recv()
    part = h0.shape[0]
    for k, held in enumerate((h0, h1, h2, h3)):
        span = pl.ds(k * part, part)
        held[...] = jnp.where(mine_ref[0] > 0, own[span, :], near[span, :])
    for k, dev in enumerate(peers):
        for copy in own_tables[k]:
            copy.wait_recv()
        forward(*table(23 + 2 * k, dev, sib, (iall.at[dev], gall.at[dev])))
    own_rows['xl'].wait_recv()
    forward(rows(19, dev_x, low, sib))
    own_rows['yh'].wait_recv()
    forward(rows(20, dev_y, high, sib))
    sent[0].wait_recv()
    forward(rows(21, dev_d, high, sib))
    sent[2].wait_recv()
    forward(rows(22, dev_d, low, sib))
    for copy in own_tables[3]:
        copy.wait_recv()
    for key in ('sl', 'sh'):
        own_rows[key].wait_recv()
    for k, copy in enumerate(sent):
        if k not in (0, 2):
            copy.wait_recv()
        copy.wait_send()
    for copy in list(own_rows.values()) + [copy for copies in own_tables for copy in copies]:
        copy.wait_send()
    slot.wait_send()
    for copy in reads:
        copy.wait()


def lands(src, dst, slot, slots):
    me = lax.axis_index('ep')
    local = (src[0] // slots == me) & (src[1] // slots == me)
    for i in range(2):
        slot = jnp.where(local & (slot == src[i] % slots), dst[i] % slots + slots, slot)
    return slot % slots


def stream(src, dst, slots0, w, w_new, bufs, sem_in, sem_out):
    def load(i):
        return [pltpu.make_async_copy(w[k].at[slots0 + i], bufs[k].at[i], sem_in.at[k, i]) for k in range(3)]

    def drain(i):
        to = lands(src, dst, slots0 + i, w[0].shape[0])
        return [pltpu.make_async_copy(bufs[k].at[i], w_new[k].at[to], sem_out.at[k, i]) for k in range(3)]

    return load, drain


def experts(i, xs, gate, bufs):
    act_g = jnp.dot(xs, bufs[0][i], preferred_element_type=F32)
    act_u = jnp.dot(xs, bufs[1][i], preferred_element_type=F32)
    z = (jax.nn.silu(act_g) * act_u).astype(BF16)
    o = jnp.dot(z, bufs[2][i], preferred_element_type=F32)
    return (o * gate).astype(BF16)


def first_kernel(src, dst, old_map, x_ref, iall, gall, *rest):
    bufs, rest = rest[:-21], rest[-21:]
    wg, wu, wd, wg_new, wu_new, wd_new, xg_out, at_ref, gr_out, c_ref, eg, eu, ed, xg, a_ref, gr_ref, pos, gsc = rest[:18]
    more_in, more_out, sem_out = rest[18:]
    me = lax.axis_index('ep')
    slots, tok, cap = wg_new.shape[0], 64, 8
    total = x_ref.shape[0]
    devs = total // tok
    rows = devs * cap
    done = FIRST * rows
    more = (eg, eu, ed)
    load, drain = stream(src, dst, EARLY, (wg, wu, wd), (wg_new, wu_new, wd_new), more, more_in, more_out)
    for i in range(FIRST - EARLY):
        for copy in load(i):
            copy.start()
    held = len(bufs) // 3
    size = EARLY // held
    drains = [pltpu.make_async_copy(bufs[k * held + i].at[0], new.at[lands(src, dst, i, slots)], sem_out.at[k, i])
              for i in range(held) for k, new in enumerate((wg_new, wu_new, wd_new))]
    for copy in drains:
        copy.start()

    ids = jnp.concatenate([iall[d].astype(F32) for d in range(devs)], axis=1)
    gates = jnp.concatenate([gall[d] for d in range(devs)], axis=1)
    hits, gs = [], []
    for j in range(slots):
        same = ids == old_map[me * slots + j].astype(F32)
        hits.append(jnp.sum(jnp.where(same, 1.0, 0.0), axis=0, keepdims=True))
        gs.append(jnp.sum(jnp.where(same, gates, 0.0), axis=0, keepdims=True))
    hit = jnp.concatenate(hits, axis=0)
    gsc[...] = jnp.concatenate(gs, axis=0)
    t_row = lax.broadcasted_iota(jnp.int32, (total, total), 0)
    t_col = lax.broadcasted_iota(jnp.int32, (total, total), 1)
    before = jnp.where((t_row < t_col) & (t_row // tok == t_col // tok), 1.0, 0.0).astype(BF16)
    rank = jnp.dot(hit.astype(BF16), before, preferred_element_type=F32)
    owner = (lax.broadcasted_iota(jnp.int32, (slots, total), 1) // tok * cap).astype(F32)
    pos[...] = jnp.where(hit > 0.5, rank + owner, -1.0)
    post = jnp.transpose(jnp.concatenate([pos[...], jnp.full((128 - slots, total), -1.0, F32)], axis=0))
    wide = lax.broadcasted_iota(jnp.int32, (total, 128), 1)
    for p in range(slots // 2):
        want = jnp.where(wide < rows, post[:, 2 * p:2 * p + 1], post[:, 2 * p + 1:2 * p + 2])
        at_ref[:, pl.ds(128 * p, 128)] = jnp.where(want == (wide % rows).astype(F32), 1.0, 0.0).astype(BF16)

    row_id = lax.broadcasted_iota(jnp.int32, (rows, total), 0).astype(F32)

    def choose(first, count, g_ref):
        @pl.loop(0, count)
        def _(j):
            chosen = row_id == pos[pl.ds(first + j, 1), :]
            a_ref[pl.ds(pl.multiple_of((first + j) * rows, rows), rows), :] = jnp.where(chosen, 1.0, 0.0).astype(BF16)
            g = jnp.sum(jnp.where(chosen, gsc[pl.ds(first + j, 1), :], 0.0), axis=1, keepdims=True)
            g_ref[pl.ds(pl.multiple_of(j * rows, rows), rows), :] = jnp.broadcast_to(g, (rows, 128))

    def gather(first, count, to_ref):
        step = max(d for d in range(16, 257, 16) if count % d == 0)

        @pl.loop(0, count // step)
        def _(q):
            r0 = pl.multiple_of(q * step, step)
            picked = jnp.dot(a_ref[pl.ds(first + r0, step), :], x_ref[...], preferred_element_type=F32)
            to_ref[pl.ds(r0, step), :] = picked.astype(BF16)

    choose(0, FIRST, gr_ref)
    gather(0, done, xg)

    for n in range(held):
        @pl.loop(0, size)
        def _(i):
            at = pl.ds(pl.multiple_of((n * size + i) * rows, rows), rows)
            c_ref[at, :] = experts(i, xg[at, :], gr_ref[at, 0:1], bufs[n::held])

    @pl.loop(0, FIRST - EARLY)
    def _(i):
        for copy in load(i):
            copy.wait()
        for copy in drain(i):
            copy.start()
        at = pl.ds(pl.multiple_of((EARLY + i) * rows, rows), rows)
        c_ref[at, :] = experts(i, xg[at, :], gr_ref[at, 0:1], more)

    choose(FIRST, slots - FIRST, gr_out)
    gather(done, (slots - FIRST) * rows, xg_out)
    for copy in drains:
        copy.wait()
    for i in range(FIRST - EARLY):
        for copy in drain(i):
            copy.wait()


def later(src, dst, first_slot, xg, gr_ref, w, w_new, c_ref, c_base, bufs, sem_in, sem_out, begin, finish):
    count = bufs[0].shape[0]
    rows = gr_ref.shape[0] // (w[0].shape[0] - FIRST)
    load, drain = stream(src, dst, first_slot, w, w_new, bufs, sem_in, sem_out)
    for i in range(count):
        for copy in load(i):
            copy.start()
    base = (first_slot - FIRST) * rows
    begin()

    @pl.loop(0, count)
    def _(i):
        for copy in load(i):
            copy.wait()
        for copy in drain(i):
            copy.start()
        r0 = pl.multiple_of(i * rows, rows)
        at = pl.ds(pl.multiple_of(base + r0, rows), rows)
        c_ref[pl.ds(pl.multiple_of(c_base + r0, rows), rows), :] = experts(i, xg[at, :], gr_ref[at, 0:1], bufs)

    finish()
    for i in range(count):
        for copy in drain(i):
            copy.wait()


def second_kernel(src, dst, xg, gr_ref, wg, wu, wd, wg_old, wu_old, wd_old, wg_new, wu_new, wd_new, c_ref,
                  bg, bu, bd, sem_in, sem_out):
    later(src, dst, FIRST, xg, gr_ref, (wg, wu, wd), (wg_new, wu_new, wd_new), c_ref, 0, (bg, bu, bd), sem_in, sem_out,
          lambda: None, lambda: None)


def third_kernel(src, dst, xg, gr_ref, at_ref, c0, c1, wg, wu, wd, wg_old, wu_old, wd_old, wg_new, wu_new, wd_new, out_ref,
                 bg, bu, bd, c_ref, sem_in, sem_out):
    cols = 256
    n0 = c0.shape[0]
    done = n0 + c1.shape[0]

    def over_columns(sums):
        @pl.loop(0, out_ref.shape[1] // cols)
        def _(n):
            at = pl.ds(pl.multiple_of(n * cols, cols), cols)
            out_ref[:, at] = sums(at)

    def begin():
        over_columns(lambda at: jnp.dot(at_ref[:, 0:n0], c0[:, at], preferred_element_type=F32)
                     + jnp.dot(at_ref[:, n0:done], c1[:, at], preferred_element_type=F32))

    def finish():
        over_columns(lambda at: out_ref[:, at] + jnp.dot(at_ref[:, done:], c_ref[:, at], preferred_element_type=F32))

    later(src, dst, FIRST + SECOND, xg, gr_ref, (wg, wu, wd), (wg_new, wu_new, wd_new), c_ref, 0, (bg, bu, bd), sem_in, sem_out,
          begin, finish)


def combine_kernel(part, x_ref, rx1, rx2, rx3, ry1, ry2, ry3, own, y_ref, got, gown, near, summed, far, relay, last,
                   send, recv):
    me, core, chip, sib, chips = places()
    dev_x, dev_y = chips[1] * 2 + core, chips[2] * 2 + core
    order = list(chips) + [chip]
    enter([dev_x, dev_y, sib])
    half = x_ref.shape[1] // 2
    cols = (pl.ds(0, half), pl.ds(half, half))
    early = [remote(part.at[order[0] * 2 + 1 - core, :, at], near.at[0, :, at], send.at[k], recv.at[k], sib)
             for k, at in zip((0, 17), cols)]
    across = early + [remote(part.at[order[k] * 2 + 1 - core], near.at[k], send.at[k], recv.at[k], sib) for k in range(1, 4)]
    for copy in across:
        copy.start()
    moved = [remote(r, got.at[k], send.at[10 + k], recv.at[10 + k], sib) for k, r in enumerate((rx1, rx2, rx3, ry1, ry2, ry3))]
    moved.append(remote(own, gown, send.at[16], recv.at[16], sib))
    for copy in moved:
        copy.start()
    towards = (dev_x, dev_y)
    diag = [remote(summed.at[0, :, cols[h]], far.at[0, :, cols[h]], send.at[4 + h], recv.at[4 + h], towards[h]) for h in range(2)]
    next_ = [remote(summed.at[1 + h, :, cols[h]], far.at[1, :, cols[h]], send.at[6 + h], recv.at[6 + h], towards[h]) for h in range(2)]
    onward = [remote(relay.at[h], last.at[h], send.at[8 + h], recv.at[8 + h], towards[1 - h]) for h in range(2)]
    for h in range(2):
        early[h].wait_recv()
        summed[0, :, cols[h]] = part[order[0] * 2 + core, :, cols[h]] + near[0, :, cols[h]]
        diag[h].start()
    for k in range(1, 4):
        across[k + 1].wait_recv()
        summed[k] = part[order[k] * 2 + core] + near[k]
        if k < 3:
            next_[k - 1].start()
    acc = x_ref[...].astype(F32) + summed[3]
    for h in range(2):
        diag[h].wait_recv()
        relay[h] = summed[2 - h, :, cols[h]] + far[0, :, cols[h]]
    for h in range(2):
        onward[h].start()
    for h in range(2):
        next_[h].wait_recv()
    acc = acc + far[1]
    for h in range(2):
        onward[h].wait_recv()
        y_ref[:, cols[h]] = (acc[:, h * half:(h + 1) * half] + last[h]).astype(BF16)
    for copy in moved:
        copy.wait_recv()
    for copy in across + diag + next_ + onward + moved:
        copy.wait_send()


def patch_kernel(dst, y_ref, rx1, rx2, rx3, ry1, ry2, ry3, got, near, gown, wg_old, wu_old, wd_old,
                 wg_new, wu_new, wd_new, y_out, sem):
    put_y = pltpu.make_async_copy(y_ref, y_out, sem.at[13])
    put_y.start()
    me = lax.axis_index('ep')
    core = me % 2
    slots, depth, width = wg_new.shape
    part = rx1.shape[0]
    count = 3 * depth // part
    owner = [dst[i] // slots for i in range(2)]
    here = [owner[i] == me for i in range(2)]
    chip = [owner[i] // 2 for i in range(2)]
    local = here[0] & here[1]
    comes = (here[0] | here[1]) & jnp.logical_not(local)
    same_x, same_y = chip[0] % 2 == chip[1] % 2, chip[0] // 2 == chip[1] // 2

    def put(refs, slot):
        spans = [(0, depth, wg_new, None), (depth, 2 * depth, wu_new, None)]
        spans += [(2 * depth + width * b, 2 * depth + width * (b + 1), wd_new, b) for b in range(depth // width)]
        copies, at = [], 0
        for ref in refs:
            n = ref.shape[0]
            for lo, hi, new, b in spans:
                r0, r1 = max(at, lo), min(at + n, hi)
                if r0 < r1:
                    rows = pl.ds(r0 - lo, r1 - r0)
                    where = new.at[slot, rows] if b is None else new.at[slot, rows, pl.ds(width * b, width)]
                    copies.append(pltpu.make_async_copy(ref.at[pl.ds(r0 - at, r1 - r0)], where, sem.at[len(copies)]))
            at += n
        for copy in copies:
            copy.start()
        for copy in copies:
            copy.wait()

    def receive(case, mine, theirs):
        for c in range(2):
            @pl.when(comes & case & (core == c))
            def _(refs=mine + theirs if c == 0 else theirs + mine):
                put(refs, jnp.where(here[0], dst[0], dst[1]) % slots)

    no = jnp.logical_not
    came = (rx1, rx2, rx3, ry1, ry2, ry3)
    for case, order in ((same_y & no(same_x), (0, 1, 2, 5)), (same_x & no(same_y), (2, 5, 4, 3)),
                        (no(same_x) & no(same_y), (4, 5, 2, 1))):
        receive(case, [came[k] for k in order], [got.at[k] for k in order])
    receive(same_y & same_x, [near], [gown])

    put_y.wait()


def cost(flops, moved):
    return pl.CostEstimate(flops=flops, bytes_accessed=moved, transcendentals=0)


def solution(mesh):
    groups = mesh.shape['ep']

    def flip(bit):
        return [(d, d + bit - 2 * bit * ((d // bit) % 2)) for d in range(groups)]

    to_x, to_y = flip(2), flip(4)

    def local_step(x_loc, expert_ids, gate_val, w_gate, w_up, w_down, old_map, mig_src, mig_dst):
        tok, model = x_loc.shape
        top = expert_ids.shape[1]
        slots, depth, width = w_gate.shape
        total = groups * tok
        per = groups * 8
        rows = slots * per
        late = (slots - FIRST) * per
        half = 3 * depth // 2
        weights = (w_gate, w_up, w_down)
        shapes = tuple(jax.ShapeDtypeStruct(w.shape, BF16) for w in weights)
        dma = pltpu.SemaphoreType.DMA
        slot_bytes = 6 * depth * width

        def params(mib, **kw):
            return pltpu.CompilerParams(vmem_limit_bytes=mib * MIB, **kw)

        def bf(*shape):
            return jax.ShapeDtypeStruct(shape, BF16)

        i_own, chip_own, send, own = pl.pallas_call(
            pack_kernel,
            out_shape=(jax.ShapeDtypeStruct((1,), jnp.int32),) * 2 + (bf(half, width),) * 2,
            in_specs=[SMEM, HBM, HBM, HBM], out_specs=(SMEM, SMEM, VMEM, VMEM),
            scratch_shapes=[dma((6,))], compiler_params=params(42),
            cost_estimate=cost(2_000_000_000, 2 * slot_bytes), name='pack',
        )(mig_src, *weights)

        part = half // 4
        xall, iall, gall, near, h0, h1, h2, h3, *bufs = pl.pallas_call(
            dispatch_kernel,
            out_shape=(bf(groups, tok, model), jax.ShapeDtypeStruct((groups, top, tok), jnp.int32),
                       jax.ShapeDtypeStruct((groups, top, tok), F32), bf(half, width))
            + (bf(part, width),) * 4 + tuple(bf(HELD, *w.shape[1:]) for w in weights for _ in range(EARLY // HELD)),
            in_specs=[SMEM, VMEM, VMEM, VMEM, ANY, VMEM, HBM, HBM, HBM], out_specs=(VMEM,) * (8 + 3 * (EARLY // HELD)),
            scratch_shapes=[dma((29,)), dma((29,)), dma((3 * (EARLY // HELD),))],
            compiler_params=params(4, collective_id=0, has_side_effects=True),
            cost_estimate=cost(8_000_000_000, 2_000_000), name='dispatch',
        )(i_own, x_loc, expert_ids.T, gate_val.T, send, own, *weights)

        chip_own = chip_own[0] > 0
        held = (h0, h1, h2, h3)

        def hop(to_x_rows, to_y_rows):
            return lax.ppermute(to_x_rows, 'ep', to_x), lax.ppermute(to_y_rows, 'ep', to_y)

        def onward(k_x, k_y, from_x, from_y, ready):
            from_x, from_y, *ready = lax.optimization_barrier((from_x, from_y, *ready))
            rows_x, rows_y = jnp.where(chip_own, held[k_x], from_y), jnp.where(chip_own, held[k_y], from_x)
            rows_x, rows_y, *ready = lax.optimization_barrier((rows_x, rows_y, *ready))
            return from_x, from_y, *hop(rows_x, rows_y), ready

        rx1, ry1 = hop(held[0], held[3])

        def room(count):
            return [pltpu.VMEM((count,) + w.shape[1:], BF16) for w in weights]

        *new, xg, at, gr, c0 = pl.pallas_call(
            first_kernel,
            out_shape=shapes + (bf(late, model), bf(total, rows), jax.ShapeDtypeStruct((late, 128), F32), bf(FIRST * per, model)),
            in_specs=[SMEM] * 3 + [VMEM] * (3 + 3 * (EARLY // HELD)) + [HBM] * 3, out_specs=(HBM,) * 3 + (VMEM,) * 4,
            scratch_shapes=room(FIRST - EARLY) + [
                pltpu.VMEM((FIRST * per, model), BF16), pltpu.VMEM((rows, total), BF16), pltpu.VMEM((FIRST * per, 128), F32),
                pltpu.VMEM((slots, total), F32), pltpu.VMEM((slots, total), F32),
                dma((3, FIRST - EARLY)), dma((3, FIRST - EARLY)), dma((3, EARLY // HELD))],
            compiler_params=params(11), cost_estimate=cost(30_000_000_000, (2 * FIRST - EARLY) * slot_bytes), name='first',
        )(mig_src, mig_dst, old_map, xall.reshape(total, model), iall, gall, *bufs, *weights)

        rx1, ry1, rx2, ry2, (xg, c0) = onward(1, 2, rx1, ry1, (xg, c0))
        *new, c1 = pl.pallas_call(
            second_kernel,
            out_shape=shapes + (bf(SECOND * per, model),),
            in_specs=[SMEM] * 2 + [VMEM] * 2 + [HBM] * 6, out_specs=(HBM,) * 3 + (VMEM,),
            input_output_aliases={7: 0, 8: 1, 9: 2},
            scratch_shapes=room(SECOND) + [dma((3, SECOND))] * 2,
            compiler_params=params(40), cost_estimate=cost(30_000_000_000, 2 * SECOND * slot_bytes), name='second',
        )(mig_src, mig_dst, xg, gr, *weights, *new)

        rx2, ry2, rx3, ry3, (xg, c1) = onward(2, 1, rx2, ry2, (xg, c1))
        *new, psum = pl.pallas_call(
            third_kernel,
            out_shape=shapes + (jax.ShapeDtypeStruct((total, model), F32),),
            in_specs=[SMEM] * 2 + [VMEM] * 5 + [HBM] * 6, out_specs=(HBM,) * 3 + (VMEM,),
            input_output_aliases={10: 0, 11: 1, 12: 2},
            scratch_shapes=room(THIRD) + [pltpu.VMEM((THIRD * per, model), BF16)] + [dma((3, THIRD))] * 2,
            compiler_params=params(40), cost_estimate=cost(30_000_000_000, 2 * THIRD * slot_bytes), name='third',
        )(mig_src, mig_dst, xg, gr, at, c0, c1, *weights, *new)

        came = (rx1, rx2, rx3, ry1, ry2, ry3)
        y_out, got, gown = pl.pallas_call(
            combine_kernel,
            out_shape=(bf(tok, model), bf(6, part, width), bf(half, width)),
            in_specs=[VMEM, VMEM] + [ANY] * 7, out_specs=(VMEM, ANY, ANY),
            scratch_shapes=[pltpu.VMEM((4, tok, model), F32), pltpu.VMEM((4, tok, model), F32),
                            pltpu.VMEM((2, tok, model), F32), pltpu.VMEM((2, tok, model // 2), F32),
                            pltpu.VMEM((2, tok, model // 2), F32), dma((18,)), dma((18,))],
            compiler_params=params(24, collective_id=1, has_side_effects=True),
            cost_estimate=cost(16_000_000_000, 4_000_000), name='combine',
        )(psum.reshape(groups, tok, model), x_loc, *came, own)

        *new, y_out = pl.pallas_call(
            patch_kernel,
            out_shape=shapes + (bf(tok, model),),
            in_specs=[SMEM] + [VMEM] * 10 + [HBM] * 3, out_specs=(HBM,) * 4,
            input_output_aliases={11: 0, 12: 1, 13: 2},
            scratch_shapes=[dma((14,))],
            compiler_params=params(40), cost_estimate=cost(3_000_000_000, 2 * slot_bytes), name='patch',
        )(mig_dst, y_out, *came, got, near, gown, *new)
        return (y_out, *new)

    row_spec = P(('dp', 'ep'), None)
    slot_spec = P('ep', None, None)
    return jax.shard_map(local_step, mesh=mesh, in_specs=(row_spec, row_spec, row_spec, slot_spec, slot_spec, slot_spec, P(), P(), P()), out_specs=(row_spec, slot_spec, slot_spec, slot_spec), check_vma=False)
```
